32 devices in a mesh: data: 32 (over z, y, x, core).
Axes of the slice: x: 2, y: 2, z: 4, core: 2. Of those that a mesh axis runs over, the one named last changes fastest.
Arguments:
- grad_attn: bfloat16 [32, 64, 65536], P('data')
- grad_mlp: bfloat16 [32, 32, 262144], P('data')
- grad_wide: bfloat16 [32, 16, 1024], P('data')
- grad_vec: bfloat16 [32, 146, 256], P('data')
- weight_attn: float32 [64, 65536], P(None, 'data')
- weight_mlp: float32 [32, 262144], P(None, 'data')
- weight_wide: float32 [16, 1024], P(None, 'data')
- weight_vec: float32 [146, 256], P(None, 'data')
- mom1_attn: float32 [64, 65536], P(None, 'data')
- mom1_mlp: float32 [32, 262144], P(None, 'data')
- mom1_wide: float32 [16, 1024], P(None, 'data')
- mom1_vec: float32 [146, 256], P(None, 'data')
- mom2_attn: float32 [64, 65536], P(None, 'data')
- mom2_mlp: float32 [32, 262144], P(None, 'data')
- mom2_wide: float32 [16, 1024], P(None, 'data')
- mom2_vec: float32 [146, 256], P(None, 'data')
Outputs:
- output 1: bfloat16 [64, 65536], replicated
- output 2: bfloat16 [32, 262144], replicated
- output 3: bfloat16 [16, 1024], replicated
- output 4: bfloat16 [146, 256], replicated
- output 5: float32 [64, 65536], P(None, 'data')
- output 6: float32 [32, 262144], P(None, 'data')
- output 7: float32 [16, 1024], P(None, 'data')
- output 8: float32 [146, 256], P(None, 'data')
- output 9: float32 [64, 65536], P(None, 'data')
- output 10: float32 [32, 262144], P(None, 'data')
- output 11: float32 [16, 1024], P(None, 'data')
- output 12: float32 [146, 256], P(None, 'data')
- output 13: float32 [64, 65536], P(None, 'data')
- output 14: float32 [32, 262144], P(None, 'data')
- output 15: float32 [16, 1024], P(None, 'data')
- output 16: float32 [146, 256], P(None, 'data')
All inputs are finite; a program needn't handle non-finite values.
Results may differ from the reference program's by a relative error of at most 0.001.
Values are sent between devices in bfloat16 or wider.
A program may use at most 1 GiB of HBM per device.

```python
import jax
import jax.numpy as jnp

GROUP_SIZE = 32
LAYERS = 16
D = 256
FF = 1024
STEP_NUMBER = 10

LEARN_RATE = 0.04
BETA_FIRST = 0.9
BETA_SECOND = 0.999
EPSILON = 1e-6
WEIGHT_DECAY = 0.01
MAX_NORM = 1.0
TARGET_NORM = 3.0


def bank_layout():
    gain_rows = jnp.array([1.0, 0.0, 0.0, 0.0, 0.0, 0.0, 1.0, 0.0, 0.0] * LAYERS + [1.0, 0.0])
    counts = (4 * LAYERS, 2 * LAYERS, LAYERS, 9 * LAYERS + 2)
    lengths = (D * D, D * FF, FF, D)
    base_scales = (
        jnp.full((4 * LAYERS,), D ** -0.5),
        jnp.array([D ** -0.5, FF ** -0.5] * LAYERS),
        jnp.full((LAYERS,), 0.05),
        0.05 + 0.15 * gain_rows,
    )
    offsets = (jnp.zeros((4 * LAYERS,)), jnp.zeros((2 * LAYERS,)), jnp.zeros((LAYERS,)), gain_rows)
    return counts, lengths, base_scales, offsets


def setup_inputs(seed: int = 0) -> dict:
    root_key = jax.random.key(seed)
    counts, lengths, base_scales, offsets = bank_layout()
    bank_keys = [jax.random.split(jax.random.fold_in(root_key, bank_index), 6) for bank_index in range(4)]
    grad_mults = [jnp.exp(jax.random.uniform(bank_keys[bank_index][0], (counts[bank_index],), minval=-1.0, maxval=1.0)) for bank_index in range(4)]
    weighted = sum(lengths[bank_index] * jnp.sum(grad_mults[bank_index] ** 2) for bank_index in range(4))
    grad_unit = TARGET_NORM * jnp.sqrt(GROUP_SIZE / weighted)
    clip_guess = MAX_NORM / TARGET_NORM
    grad_banks, weights, firsts, seconds = [], [], [], []
    for bank_index in range(4):
        bank_keyset = bank_keys[bank_index]
        row_count = counts[bank_index]
        row_length = lengths[bank_index]
        grad_scale = grad_unit * grad_mults[bank_index]
        device_grads = jax.random.normal(bank_keyset[1], (GROUP_SIZE, row_count, row_length)) * grad_scale[None, :, None]
        grad_banks.append(device_grads.astype(jnp.bfloat16))
        weight_spread = jnp.exp(jax.random.uniform(bank_keyset[2], (row_count,), minval=-1.2, maxval=1.2))
        row_scale = base_scales[bank_index] * weight_spread
        weights.append(offsets[bank_index][:, None] + row_scale[:, None] * jax.random.normal(bank_keyset[3], (row_count, row_length)))
        moment_unit = clip_guess * grad_scale / GROUP_SIZE ** 0.5
        firsts.append(0.1 * moment_unit[:, None] * jax.random.normal(bank_keyset[4], (row_count, row_length)))
        seconds.append(0.001 * (moment_unit * moment_unit)[:, None] * jnp.exp(0.5 * jax.random.normal(bank_keyset[5], (row_count, row_length))))
    bank_names = ("attn", "mlp", "wide", "vec")
    inputs = {}
    for prefix, arrays in (("grad_", grad_banks), ("weight_", weights), ("mom1_", firsts), ("mom2_", seconds)):
        for bank_index in range(4):
            inputs[prefix + bank_names[bank_index]] = arrays[bank_index]
    return inputs


def lamb_bank(mean_grad, weight, first_moment, second_moment, clip_coef):
    clipped = clip_coef * mean_grad
    new_first = BETA_FIRST * first_moment + (1.0 - BETA_FIRST) * clipped
    new_second = BETA_SECOND * second_moment + (1.0 - BETA_SECOND) * (clipped * clipped)
    update = (new_first / (1.0 - BETA_FIRST ** STEP_NUMBER)) / (jnp.sqrt(new_second / (1.0 - BETA_SECOND ** STEP_NUMBER)) + EPSILON) + WEIGHT_DECAY * weight
    weight_norm = jnp.sqrt(jnp.sum(weight * weight, axis=1, keepdims=True))
    update_norm = jnp.sqrt(jnp.sum(update * update, axis=1, keepdims=True))
    new_weight = weight - LEARN_RATE * (weight_norm / update_norm) * update
    return new_weight.astype(jnp.bfloat16), new_weight, new_first, new_second


def reference(grad_attn, grad_mlp, grad_wide, grad_vec, weight_attn, weight_mlp, weight_wide, weight_vec, mom1_attn, mom1_mlp, mom1_wide, mom1_vec, mom2_attn, mom2_mlp, mom2_wide, mom2_vec):
    mean_attn = jnp.sum(grad_attn, axis=0, dtype=jnp.float32) / GROUP_SIZE
    mean_mlp = jnp.sum(grad_mlp, axis=0, dtype=jnp.float32) / GROUP_SIZE
    mean_wide = jnp.sum(grad_wide, axis=0, dtype=jnp.float32) / GROUP_SIZE
    mean_vec = jnp.sum(grad_vec, axis=0, dtype=jnp.float32) / GROUP_SIZE
    total_square = jnp.sum(mean_attn * mean_attn) + jnp.sum(mean_mlp * mean_mlp) + jnp.sum(mean_wide * mean_wide) + jnp.sum(mean_vec * mean_vec)
    clip_coef = jnp.minimum(1.0, MAX_NORM / jnp.sqrt(total_square))
    attn_out = lamb_bank(mean_attn, weight_attn, mom1_attn, mom2_attn, clip_coef)
    mlp_out = lamb_bank(mean_mlp, weight_mlp, mom1_mlp, mom2_mlp, clip_coef)
    wide_out = lamb_bank(mean_wide, weight_wide, mom1_wide, mom2_wide, clip_coef)
    vec_out = lamb_bank(mean_vec, weight_vec, mom1_vec, mom2_vec, clip_coef)
    return (attn_out[0], mlp_out[0], wide_out[0], vec_out[0], attn_out[1], mlp_out[1], wide_out[1], vec_out[1], attn_out[2], mlp_out[2], wide_out[2], vec_out[2], attn_out[3], mlp_out[3], wide_out[3], vec_out[3])
```

```python
import jax
import jax.numpy as jnp
from jax import lax
from jax.experimental import pallas as pl
from jax.experimental.pallas import tpu as pltpu
from jax.sharding import PartitionSpec as P

STEP_NUMBER = 10
LEARN_RATE = 0.04
BETA_FIRST = 0.9
BETA_SECOND = 0.999
EPSILON = 1e-6
WEIGHT_DECAY = 0.01
MAX_NORM = 1.0

GROUP = 32
AXIS = "data"
MESH = pl.DeviceIdType.MESH
F32 = jnp.float32
BF16 = jnp.bfloat16

ROWS = 16
WIDTH = 1024
OWN_A = 2048
OWN_M = 8192
SUB_A = OWN_A // WIDTH
SUB_M = OWN_M // WIDTH
CHUNKS_A = 4 * SUB_A
CHUNKS_M = 2 * SUB_M
CHUNKS = CHUNKS_A + CHUNKS_M
PAIRS = CHUNKS // 2
AHEAD = 2
SLOTS = 3
TILES = WIDTH // 128


def coords():
    me = lax.axis_index(AXIS)
    return me // 8, lax.rem(me // 4, 2), lax.rem(me // 2, 2), lax.rem(me, 2)


def index_of(z, y, x, c):
    return ((z * 2 + y) * 2 + x) * 2 + c


def remote(src, dst, send_sem, recv_sem, device):
    return pltpu.make_async_remote_copy(src_ref=src, dst_ref=dst, send_sem=send_sem, recv_sem=recv_sem, device_id=(device,), device_id_type=MESH)


def wait_bytes(ref, sem):
    pltpu.make_async_copy(ref, ref, sem).wait()


def bank_of(k, attn_case, mlp_case):
    @pl.when(k < CHUNKS_A)
    def _():
        attn_case(k // SUB_A, lax.rem(k, SUB_A))

    @pl.when(k >= CHUNKS_A)
    def _():
        local = k - CHUNKS_A
        mlp_case(local // SUB_M, lax.rem(local, SUB_M))


def row_group(k):
    return jnp.where(k < CHUNKS_A, k // SUB_A, 4 + (k - CHUNKS_A) // SUB_M)


def adam(gs, w, m, v, clip):
    clipped = clip * gs
    new_m = BETA_FIRST * m + (1.0 - BETA_FIRST) * clipped
    new_v = BETA_SECOND * v + (1.0 - BETA_SECOND) * (clipped * clipped)
    u = (new_m / (1.0 - BETA_FIRST ** STEP_NUMBER)) / (jnp.sqrt(new_v / (1.0 - BETA_SECOND ** STEP_NUMBER)) + EPSILON) + WEIGHT_DECAY * w
    return u, new_m, new_v


def all_to_all_small(me, start_one):
    def body(i, carry):
        start_one(lax.rem(me + 1 + i, GROUP))
        return carry
    lax.fori_loop(0, GROUP - 1, body, 0)


def step_kernel(g_attn, g_mlp, g_small, w_attn, w_mlp, m_attn, m_mlp, v_attn, v_mlp, w_small, m_small, v_small,
                land, nw, nm, nv, small_all, nw_small, nm_small, nv_small,
                acc1, s2buf, s3buf, gsum, small_in, small_u, msg, inbox1, inbox2, rows_w, rows_u, ratio, clip_tile, n_acc,
                s1_send, s1_recv, s2_send, s2_recv, s3_send, s3_recv, d_send, d_recv, load_sem, misc_send, misc_recv):
    me = lax.axis_index(AXIS)
    z, y, x, c = coords()

    def load_state(k, carry):
        def attn(rg, sub):
            for i, (src, dst) in enumerate(((w_attn, nw), (m_attn, nm), (v_attn, nv))):
                pltpu.make_async_copy(src.at[pl.ds(rg * ROWS, ROWS), pl.ds(pl.multiple_of(sub * WIDTH, 128), WIDTH)], dst.at[k], load_sem.at[i]).start()

        def mlp(rg, sub):
            for i, (src, dst) in enumerate(((w_mlp, nw), (m_mlp, nm), (v_mlp, nv))):
                pltpu.make_async_copy(src.at[pl.ds(rg * ROWS, ROWS), pl.ds(pl.multiple_of(sub * WIDTH, 128), WIDTH)], dst.at[k], load_sem.at[i]).start()
        bank_of(k, attn, mlp)
        return carry
    lax.fori_loop(0, CHUNKS, load_state, 0)

    barrier = pltpu.get_barrier_semaphore()
    all_to_all_small(me, lambda i: pl.semaphore_signal(barrier, inc=1, device_id=(i,), device_id_type=MESH))
    pl.semaphore_wait(barrier, GROUP - 1)

    def a_peer(t, da, dc):
        cc = c + dc - 2 * c * dc
        if t == 0:
            return index_of(z, y, x + da - 2 * x * da, cc)
        return index_of(z, y + da - 2 * y * da, x, cc)

    def b_peer(t):
        return index_of(z, 1 - y, x, c) if t == 0 else index_of(z, y, 1 - x, c)

    def a_of(t):
        return x if t == 0 else y

    def b_of(t):
        return y if t == 0 else x

    def first_start(j, t):
        k = 2 * j + t

        def issue(grad, rg, sub, own):
            def body(b, carry):
                bb, zz = b // 4, lax.rem(b, 4)
                for da in range(2):
                    for dc in range(2):
                        aa = a_of(t) + da - 2 * a_of(t) * da
                        cc = c + dc - 2 * c * dc
                        owner = index_of(zz, bb, aa, cc) if t == 0 else index_of(zz, aa, bb, cc)
                        src = grad.at[0, pl.ds(rg * ROWS, ROWS), pl.ds(pl.multiple_of(owner * own + sub * WIDTH, 128), WIDTH)]
                        dst = land.at[k, (da * 2 + dc) * 8 + b]
                        if da == 0 and dc == 0:
                            pltpu.make_async_copy(src, dst, s1_recv.at[k]).start()
                        else:
                            remote(src, dst, s1_send.at[k], s1_recv.at[k], a_peer(t, da, dc)).start()
                return carry
            lax.fori_loop(0, 8, body, 0)
        bank_of(k, lambda rg, sub: issue(g_attn, rg, sub, OWN_A), lambda rg, sub: issue(g_mlp, rg, sub, OWN_M))

    def first_finish(j, t):
        k = 2 * j + t
        slot = lax.rem(j, SLOTS) * 2 + t

        @pl.when(j >= SLOTS)
        def _():
            wait_bytes(s2buf.at[k - 2 * SLOTS], s2_send.at[k - 2 * SLOTS])
        wait_bytes(land.at[k], s1_recv.at[k])

        def body(b, carry):
            for i in range(TILES):
                cols = pl.ds(i * 128, 128)
                parts = [land[k, p * 8 + b, :, cols].astype(F32) for p in range(4)]
                acc1[slot, b, :, cols] = (parts[0] + parts[1]) + (parts[2] + parts[3])
            return carry
        lax.fori_loop(0, 8, body, 0)
        remote(acc1.at[slot, pl.ds((1 - b_of(t)) * 4, 4)], s2buf.at[k], s2_send.at[k], s2_recv.at[k], b_peer(t)).start()

    def second_finish(j, t):
        k = 2 * j + t
        slot = lax.rem(j, SLOTS) * 2 + t
        wait_bytes(s2buf.at[k], s2_recv.at[k])

        def body(zz, carry):
            for i in range(TILES):
                cols = pl.ds(i * 128, 128)
                s2buf[k, zz, :, cols] = s2buf[k, zz, :, cols] + acc1[slot, b_of(t) * 4 + zz, :, cols]
            return carry
        lax.fori_loop(0, 4, body, 0)
        for dz in range(1, 4):
            peer = lax.rem(z + dz, 4)
            remote(s2buf.at[k, peer], s3buf.at[k, dz - 1], s3_send.at[k], s3_recv.at[k], index_of(peer, y, x, c)).start()

    def third_finish(j, t):
        k = 2 * j + t
        wait_bytes(s3buf.at[k], s3_recv.at[k])
        total = n_acc[...]
        for i in range(TILES):
            cols = pl.ds(i * 128, 128)
            gs = ((s2buf[k, z, :, cols] + s3buf[k, 0, :, cols]) + (s3buf[k, 1, :, cols] + s3buf[k, 2, :, cols])) * (1.0 / GROUP)
            gsum[k, :, cols] = gs
            total = total + gs * gs
        n_acc[...] = total

    for j in range(AHEAD):
        for t in range(2):
            first_start(j, t)

    def small_start(i):
        remote(g_small.at[i], small_in.at[me], misc_send.at[0], misc_recv.at[0], i).start()
    all_to_all_small(me, small_start)
    small_in[me] = g_small[me]

    for i, ref in enumerate((nw, nm, nv)):
        wait_bytes(ref, load_sem.at[i])
    n_acc[...] = jnp.zeros_like(n_acc)
    rows_w[...] = jnp.zeros_like(rows_w)
    rows_u[...] = jnp.zeros_like(rows_u)

    def weight_squares(k, carry):
        total = rows_w[row_group(k)]
        for i in range(TILES):
            w = nw[k, :, pl.ds(i * 128, 128)]
            total = total + w * w
        rows_w[row_group(k)] = total
        return carry
    lax.fori_loop(0, CHUNKS, weight_squares, 0)

    def reduce_body(j, carry):
        @pl.when(j + AHEAD < PAIRS)
        def _():
            for t in range(2):
                first_start(j + AHEAD, t)

        @pl.when(j < PAIRS)
        def _():
            for t in range(2):
                first_finish(j, t)

        @pl.when(jnp.logical_and(j >= 1, j < PAIRS + 1))
        def _():
            for t in range(2):
                second_finish(j - 1, t)

        @pl.when(j >= 2)
        def _():
            for t in range(2):
                third_finish(j - 2, t)
        return carry
    lax.fori_loop(0, PAIRS + 2, reduce_body, 0)

    wait_bytes(small_in.at[pl.ds(0, GROUP - 1)], misc_recv.at[0])
    wait_bytes(small_in.at[pl.ds(0, GROUP - 1)], misc_send.at[0])
    gs_small = jnp.sum(small_in[...], axis=0) * (1.0 / GROUP)

    sub_iota = lax.broadcasted_iota(jnp.int32, (8, 128), 0)
    eye = lax.broadcasted_iota(jnp.int32, (96, 128), 0) == lax.broadcasted_iota(jnp.int32, (96, 128), 1)

    def to_row(column_parts):
        sums = jnp.sum(column_parts, axis=1, keepdims=True)
        return jnp.sum(jnp.where(eye, jnp.broadcast_to(sums, (96, 128)), 0.0), axis=0, keepdims=True)

    def message(row0, small, row3):
        half = jnp.sum(small, axis=0, keepdims=True)
        return (jnp.where(sub_iota == 0, jnp.broadcast_to(row0, (8, 128)), 0.0)
                + jnp.where(sub_iota == 1, jnp.broadcast_to(half[:, :128], (8, 128)), 0.0)
                + jnp.where(sub_iota == 2, jnp.broadcast_to(half[:, 128:], (8, 128)), 0.0)
                + jnp.where(sub_iota == 3, jnp.broadcast_to(row3, (8, 128)), 0.0))

    def sum_over_devices(value, slot, inbox):
        msg[slot] = value
        inbox[me] = value

        def start(i):
            remote(msg.at[slot], inbox.at[me], misc_send.at[1 + slot], misc_recv.at[1 + slot], i).start()
        all_to_all_small(me, start)
        wait_bytes(inbox.at[pl.ds(0, GROUP - 1)], misc_recv.at[1 + slot])
        wait_bytes(inbox.at[pl.ds(0, GROUP - 1)], misc_send.at[1 + slot])
        return jnp.sum(inbox[...], axis=0)

    small_w = w_small[...]
    small_sq = gs_small * gs_small
    square_row = jnp.sum(n_acc[...], axis=0, keepdims=True) + jnp.sum(small_sq[:, :128], axis=0, keepdims=True) + jnp.sum(small_sq[:, 128:], axis=0, keepdims=True)
    first_sums = sum_over_devices(message(to_row(rows_w[...].reshape(96, 128)), small_w * small_w, square_row), 0, inbox1)
    clip = jnp.minimum(1.0, MAX_NORM / jnp.sqrt(jnp.sum(first_sums[3:4], axis=1, keepdims=True)))
    clip_tile[...] = jnp.broadcast_to(clip, (ROWS, 128))

    def direction(k, carry):
        cl = clip_tile[...]
        total = rows_u[row_group(k)]
        for i in range(TILES):
            cols = pl.ds(i * 128, 128)
            u, m1, v1 = adam(gsum[k, :, cols], nw[k, :, cols], nm[k, :, cols], nv[k, :, cols], cl)
            nm[k, :, cols] = m1
            nv[k, :, cols] = v1
            gsum[k, :, cols] = u
            total = total + u * u
        rows_u[row_group(k)] = total
        return carry
    lax.fori_loop(0, CHUNKS, direction, 0)
    u_small, m1_small, v1_small = adam(gs_small, small_w, m_small[...], v_small[...], jnp.broadcast_to(clip, (8, 256)))
    nm_small[...] = m1_small
    nv_small[...] = v1_small
    second_sums = sum_over_devices(message(to_row(rows_u[...].reshape(96, 128)), u_small * u_small, jnp.zeros((1, 128), F32)), 1, inbox2)

    ratio_row = jnp.sqrt(first_sums[0:1]) / jnp.sqrt(second_sums[0:1])
    ratio_col = jnp.sum(jnp.where(eye, jnp.broadcast_to(ratio_row, (96, 128)), 0.0), axis=1, keepdims=True)
    ratio[...] = jnp.broadcast_to(LEARN_RATE * ratio_col, (96, 128)).reshape(6, ROWS, 128)

    lane = lax.broadcasted_iota(jnp.int32, (1, 128), 1)

    def small_totals(sums):
        upper = sums[2:3]
        wide = jnp.where(lane >= 64, upper, 0.0)
        for shift in (64, 32, 16):
            wide = wide + pltpu.roll(wide, shift, 1)
        return sums[1:2], jnp.where(lane >= 64, wide, upper)

    w_low, w_high = small_totals(first_sums)
    u_low, u_high = small_totals(second_sums)
    r_low = LEARN_RATE * (jnp.sqrt(w_low) / jnp.sqrt(u_low))
    r_high = LEARN_RATE * (jnp.sqrt(w_high) / jnp.sqrt(u_high))
    r_small = jnp.concatenate([jnp.broadcast_to(r_low, (8, 128)), jnp.broadcast_to(r_high, (8, 128))], axis=1)
    new_small = small_w - r_small * u_small
    nw_small[...] = new_small
    small_u[...] = new_small
    small_all[me] = new_small

    def small_gather(i):
        remote(small_u, small_all.at[me], misc_send.at[3], misc_recv.at[3], i).start()
    all_to_all_small(me, small_gather)

    def gather_z(j, t):
        k = 2 * j + t
        mine = a_of(t) * 16 + c * 8 + b_of(t) * 4 + z
        rr = ratio[row_group(k)]
        for i in range(TILES):
            cols = pl.ds(i * 128, 128)
            w1 = nw[k, :, cols] - rr * gsum[k, :, cols]
            nw[k, :, cols] = w1
            land[k, mine, :, cols] = w1.astype(BF16)
        for dz in range(1, 4):
            remote(land.at[k, mine], land.at[k, mine], s3_send.at[k], s3_recv.at[k], index_of(lax.rem(z + dz, 4), y, x, c)).start()

    def gather_b(j, t):
        k = 2 * j + t
        wait_bytes(land.at[k, pl.ds(0, 3)], s3_recv.at[k])
        part = land.at[k, pl.ds(a_of(t) * 16 + c * 8 + b_of(t) * 4, 4)]
        remote(part, part, s2_send.at[k], s2_recv.at[k], b_peer(t)).start()

    def gather_a(j, t):
        k = 2 * j + t
        wait_bytes(land.at[k, pl.ds(0, 4)], s2_recv.at[k])
        part = land.at[k, pl.ds(a_of(t) * 16 + c * 8, 8)]
        remote(part, part, s1_send.at[k], s1_recv.at[k], a_peer(t, 1, 0)).start()
        remote(part, part, d_send.at[k], d_recv.at[k], a_peer(t, 0, 1)).start()

    def gather_core(j, t):
        k = 2 * j + t
        wait_bytes(land.at[k, pl.ds(0, 8)], s1_recv.at[k])
        part = land.at[k, pl.ds((1 - a_of(t)) * 16 + c * 8, 8)]
        remote(part, part, d_send.at[k], d_recv.at[k], a_peer(t, 0, 1)).start()

    def gather_body(j, carry):
        @pl.when(j < PAIRS)
        def _():
            for t in range(2):
                gather_z(j, t)

        @pl.when(jnp.logical_and(j >= 1, j < PAIRS + 1))
        def _():
            for t in range(2):
                gather_b(j - 1, t)

        @pl.when(jnp.logical_and(j >= 2, j < PAIRS + 2))
        def _():
            for t in range(2):
                gather_a(j - 2, t)

        @pl.when(j >= 3)
        def _():
            for t in range(2):
                gather_core(j - 3, t)
        return carry

    def drain_reduce(k, carry):
        wait_bytes(land.at[k, pl.ds(0, 24)], s1_send.at[k])

        @pl.when(k >= CHUNKS - 2 * SLOTS)
        def _():
            wait_bytes(s2buf.at[k], s2_send.at[k])
        wait_bytes(s3buf.at[k], s3_send.at[k])
        return carry
    lax.fori_loop(0, CHUNKS, drain_reduce, 0)
    lax.fori_loop(0, PAIRS + 3, gather_body, 0)

    def drain_gather(k, carry):
        wait_bytes(land.at[k, pl.ds(0, 16)], d_recv.at[k])
        wait_bytes(land.at[k, pl.ds(0, 16)], d_send.at[k])
        wait_bytes(land.at[k, pl.ds(0, 8)], s1_send.at[k])
        wait_bytes(land.at[k, pl.ds(0, 4)], s2_send.at[k])
        wait_bytes(land.at[k, pl.ds(0, 3)], s3_send.at[k])
        return carry
    lax.fori_loop(0, CHUNKS, drain_gather, 0)
    wait_bytes(small_all.at[pl.ds(0, GROUP - 1)], misc_recv.at[3])
    wait_bytes(small_all.at[pl.ds(0, GROUP - 1)], misc_send.at[3])


def store_kernel(land, nw, nm, nv, rep_attn, rep_mlp, w_attn, w_mlp, m_attn, m_mlp, v_attn, v_mlp, sem):
    state_out = ((nw, w_attn, w_mlp), (nm, m_attn, m_mlp), (nv, v_attn, v_mlp))

    def pair_body(j, carry):
        for t in range(2):
            k = 2 * j + t

            def issue(rep, which, own, rg, sub):
                def body(q, carry):
                    aa, cc, bb, zz = q // 16, lax.rem(q // 8, 2), lax.rem(q // 4, 2), lax.rem(q, 4)
                    owner = index_of(zz, bb, aa, cc) if t == 0 else index_of(zz, aa, bb, cc)
                    pltpu.make_async_copy(land.at[k, q], rep.at[pl.ds(rg * ROWS, ROWS), pl.ds(pl.multiple_of(owner * own + sub * WIDTH, 128), WIDTH)], sem.at[0]).start()
                    return carry
                lax.fori_loop(0, 32, body, 0, unroll=4)
                for i, refs in enumerate(state_out):
                    pltpu.make_async_copy(refs[0].at[k], refs[1 + which].at[pl.ds(rg * ROWS, ROWS), pl.ds(pl.multiple_of(sub * WIDTH, 128), WIDTH)], sem.at[1 + i]).start()
            bank_of(k, lambda rg, sub: issue(rep_attn, 0, OWN_A, rg, sub), lambda rg, sub: issue(rep_mlp, 1, OWN_M, rg, sub))
        return carry
    lax.fori_loop(0, PAIRS, pair_body, 0)
    wait_bytes(land, sem.at[0])
    for i, refs in enumerate(state_out):
        wait_bytes(refs[0], sem.at[1 + i])


def pack_small(vec, wide, fill):
    lead = vec.shape[:-2]
    vec_t = jnp.swapaxes(vec, -1, -2)
    wide_t = jnp.moveaxis(wide.reshape(lead + (16, 4, 8)), (-3, -2, -1), (-1, -2, -3)).reshape(lead + (8, 64))
    pad = jnp.full(lead + (8, 46), fill, vec.dtype)
    return jnp.concatenate([vec_t, pad, wide_t], axis=-1)


def unpack_small(packed):
    lead = packed.shape[:-2]
    vec = jnp.swapaxes(packed[..., :146], -1, -2)
    wide = jnp.moveaxis(packed[..., 192:].reshape(lead + (8, 4, 16)), (-3, -2, -1), (-1, -2, -3)).reshape(lead + (16, 32))
    return vec, wide


def solution(mesh):
    grad_spec = P(AXIS, None, None)
    shard_spec = P(None, AXIS)
    full_spec = P(None, None)

    def local_step(g_attn, g_mlp, g_wide, g_vec, w_attn, w_mlp, w_wide, w_vec, m_attn, m_mlp, m_wide, m_vec, v_attn, v_mlp, v_wide, v_vec):
        g_small = pack_small(jnp.moveaxis(g_vec.reshape(146, GROUP, 8), 1, 0), jnp.moveaxis(g_wide.reshape(16, GROUP, 32), 1, 0), 0.0).astype(F32)
        w_small = pack_small(w_vec, w_wide, 1.0)
        m_small = pack_small(m_vec, m_wide, 0.0)
        v_small = pack_small(v_vec, v_wide, 1.0)
        hbm = pl.BlockSpec(memory_space=pl.ANY)
        vmem = pl.BlockSpec(memory_space=pltpu.VMEM)
        block = (CHUNKS, ROWS, WIDTH)
        small = jax.ShapeDtypeStruct((8, 256), F32)
        dma = pltpu.SemaphoreType.DMA
        land, nw, nm, nv, small_all, nw_small, nm_small, nv_small = pl.pallas_call(
            step_kernel,
            out_shape=(pltpu.VMEM((CHUNKS, 32, ROWS, WIDTH), BF16), pltpu.VMEM(block, F32), pltpu.VMEM(block, F32), pltpu.VMEM(block, F32),
                       pltpu.VMEM((GROUP, 8, 256), F32), small, small, small),
            in_specs=[hbm, hbm, vmem] + [hbm] * 6 + [vmem] * 3,
            out_specs=(vmem,) * 8,
            scratch_shapes=[
                pltpu.VMEM((2 * SLOTS, 8, ROWS, WIDTH), F32),
                pltpu.VMEM((CHUNKS, 4, ROWS, WIDTH), F32),
                pltpu.VMEM((CHUNKS, 3, ROWS, WIDTH), F32),
                pltpu.VMEM(block, F32),
                pltpu.VMEM((GROUP, 8, 256), F32),
                pltpu.VMEM((8, 256), F32),
                pltpu.VMEM((2, 8, 128), F32),
                pltpu.VMEM((GROUP, 8, 128), F32),
                pltpu.VMEM((GROUP, 8, 128), F32),
                pltpu.VMEM((6, ROWS, 128), F32),
                pltpu.VMEM((6, ROWS, 128), F32),
                pltpu.VMEM((6, ROWS, 128), F32),
                pltpu.VMEM((ROWS, 128), F32),
                pltpu.VMEM((ROWS, 128), F32),
                dma((CHUNKS,)), dma((CHUNKS,)), dma((CHUNKS,)), dma((CHUNKS,)), dma((CHUNKS,)), dma((CHUNKS,)), dma((CHUNKS,)), dma((CHUNKS,)),
                dma((3,)), dma((4,)), dma((4,)),
            ],
            compiler_params=pltpu.CompilerParams(collective_id=0, has_side_effects=True, vmem_limit_bytes=26 * 1024 * 1024),
            name="lamb_step",
        )(g_attn, g_mlp, g_small, w_attn, w_mlp, m_attn, m_mlp, v_attn, v_mlp, w_small, m_small, v_small)
        shard_a = jax.ShapeDtypeStruct((64, OWN_A), F32)
        shard_m = jax.ShapeDtypeStruct((32, OWN_M), F32)
        rep_attn, rep_mlp, nw_attn, nw_mlp, nm_attn, nm_mlp, nv_attn, nv_mlp = pl.pallas_call(
            store_kernel,
            out_shape=(jax.ShapeDtypeStruct((64, OWN_A * GROUP), BF16), jax.ShapeDtypeStruct((32, OWN_M * GROUP), BF16),
                       shard_a, shard_m, shard_a, shard_m, shard_a, shard_m),
            in_specs=[vmem] * 4,
            out_specs=(hbm,) * 8,
            scratch_shapes=[dma((4,))],
            compiler_params=pltpu.CompilerParams(vmem_limit_bytes=4 * 1024 * 1024),
            name="store_results",
        )(land, nw, nm, nv)
        rep_vec, rep_wide = unpack_small(small_all.astype(BF16))
        rep_vec = jnp.moveaxis(rep_vec, 0, 1).reshape(146, 256)
        rep_wide = jnp.moveaxis(rep_wide, 0, 1).reshape(16, 1024)
        nw_vec, nw_wide = unpack_small(nw_small)
        nm_vec, nm_wide = unpack_small(nm_small)
        nv_vec, nv_wide = unpack_small(nv_small)
        return (rep_attn, rep_mlp, rep_wide, rep_vec, nw_attn, nw_mlp, nw_wide, nw_vec, nm_attn, nm_mlp, nm_wide, nm_vec, nv_attn, nv_mlp, nv_wide, nv_vec)

    return jax.shard_map(local_step, mesh=mesh, in_specs=(grad_spec,) * 4 + (shard_spec,) * 12, out_specs=(full_spec,) * 4 + (shard_spec,) * 12, check_vma=False)
```

```python
import jax
import jax.numpy as jnp
from jax import lax
from jax.experimental import pallas as pl
from jax.experimental.pallas import tpu as pltpu
from jax.sharding import PartitionSpec as P

STEP_NUMBER = 10
LEARN_RATE = 0.04
BETA_FIRST = 0.9
BETA_SECOND = 0.999
EPSILON = 1e-6
WEIGHT_DECAY = 0.01
MAX_NORM = 1.0

GROUP = 32
AXIS = "data"
MESH = pl.DeviceIdType.MESH
F32 = jnp.float32
BF16 = jnp.bfloat16

ROWS = 16
WIDTH = 1024
OWN_A = 2048
OWN_M = 8192
SUB_A = OWN_A // WIDTH
SUB_M = OWN_M // WIDTH
CHUNKS_A = 4 * SUB_A
CHUNKS_M = 2 * SUB_M
CHUNKS = CHUNKS_A + CHUNKS_M
PAIRS = CHUNKS // 2
AHEAD = 2
SLOTS = 3
TILES = WIDTH // 128


def coords():
    me = lax.axis_index(AXIS)
    return me // 8, lax.rem(me // 4, 2), lax.rem(me // 2, 2), lax.rem(me, 2)


def index_of(z, y, x, c):
    return ((z * 2 + y) * 2 + x) * 2 + c


def remote(src, dst, send_sem, recv_sem, device):
    return pltpu.make_async_remote_copy(src_ref=src, dst_ref=dst, send_sem=send_sem, recv_sem=recv_sem, device_id=(device,), device_id_type=MESH)


def wait_bytes(ref, sem):
    pltpu.make_async_copy(ref, ref, sem).wait()


def bank_of(k, attn_case, mlp_case):
    @pl.when(k < CHUNKS_A)
    def _():
        attn_case(k // SUB_A, lax.rem(k, SUB_A))

    @pl.when(k >= CHUNKS_A)
    def _():
        local = k - CHUNKS_A
        mlp_case(local // SUB_M, lax.rem(local, SUB_M))


def row_group(k):
    return jnp.where(k < CHUNKS_A, k // SUB_A, 4 + (k - CHUNKS_A) // SUB_M)


def adam(gs, w, m, v, clip):
    clipped = clip * gs
    new_m = BETA_FIRST * m + (1.0 - BETA_FIRST) * clipped
    new_v = BETA_SECOND * v + (1.0 - BETA_SECOND) * (clipped * clipped)
    u = (new_m * (1.0 / (1.0 - BETA_FIRST ** STEP_NUMBER))) / (jnp.sqrt(new_v * (1.0 / (1.0 - BETA_SECOND ** STEP_NUMBER))) + EPSILON) + WEIGHT_DECAY * w
    return u, new_m, new_v


def to_others(me, start_one):
    def body(i, carry):
        start_one(lax.rem(me + 1 + i, GROUP))
        return carry
    lax.fori_loop(0, GROUP - 1, body, 0)


def flip(bit, other):
    return bit + other - 2 * bit * other


def pack_state(vec_ref, wide_ref, flat, square, fill):
    flat[...] = jnp.zeros_like(flat)
    flat[0:8, 0:146] = vec_ref[...]
    square[...] = jnp.zeros_like(square)
    square[0:16, 0:32] = wide_ref[...]
    vec = flat[...]
    wide_t = square[...].T
    wide = pltpu.roll(wide_t[0:8], 64, 1)
    for g in range(1, 4):
        wide = wide + pltpu.roll(wide_t[8 * g:8 * g + 8], 64 + 16 * g, 1)
    lane = lax.broadcasted_iota(jnp.int32, (8, 256), 1)
    packed = jnp.concatenate([vec[:, :128], vec[:, 128:] + wide], axis=1)
    return jnp.where(jnp.logical_and(lane >= 146, lane < 192), fill, packed)


def unpack_state(packed, vec_ref, wide_ref, square):
    vec_ref[...] = packed[:, 0:146]
    square[...] = jnp.zeros_like(square)
    for g in range(4):
        square[8 * g:8 * g + 8, :] = pltpu.roll(packed[:, 128:], (64 - 16 * g) % 128, 1)
    wide_ref[...] = square[...].T[0:16, 0:32]


def pack_grads(g_vec, g_wide, g_small, big, long):
    big[...] = jnp.zeros_like(big)
    big[0:146, :] = g_vec[0].astype(F32)
    long[...] = jnp.zeros_like(long)
    long[0:16, :] = g_wide[0].astype(F32)
    vec = big[...].T
    wide_t = long[...].T.reshape(GROUP, 4, 8, 128)
    wide = pltpu.roll(wide_t[:, 0].reshape(GROUP * 8, 128), 64, 1)
    for g in range(1, 4):
        wide = wide + pltpu.roll(wide_t[:, g].reshape(GROUP * 8, 128), 64 + 16 * g, 1)
    g_small[:, :, 0:128] = vec[:, :128].reshape(GROUP, 8, 128)
    g_small[:, :, 128:256] = (vec[:, 128:] + wide).reshape(GROUP, 8, 128)


def unpack_replica(small_all, rep_vec, rep_wide):
    rep_vec[...] = small_all[...].reshape(GROUP * 8, 256).T[0:146].astype(BF16)
    upper = small_all[:, :, 128:256].reshape(GROUP * 8, 128)
    parts = [pltpu.roll(upper, (64 - 16 * g) % 128, 1).reshape(GROUP, 1, 8, 128) for g in range(4)]
    rep_wide[...] = jnp.concatenate(parts, axis=1).reshape(GROUP * 32, 128).T[0:16].astype(BF16)


def step_kernel(g_attn, g_mlp, g_vec, g_wide, w_attn, w_mlp, m_attn, m_mlp, v_attn, v_mlp, w_vec, w_wide, m_vec, m_wide, v_vec, v_wide,
                land, nw, nm, nv, rep_vec, rep_wide, nw_vec, nw_wide, nm_vec, nm_wide, nv_vec, nv_wide,
                acc1, s2buf, s3buf, s4buf, gsum, g_small, small_in, small_all, small_new, state_small, big, long, flat, square,
                msg, inbox1, inbox2, rows_w, rows_u, ratio, clip_tile, n_acc,
                s1_send, s1_recv, s2_send, s2_recv, s3_send, s3_recv, s4_send, s4_recv, d_send, d_recv, load_sem, misc_send, misc_recv):
    me = lax.axis_index(AXIS)
    z, y, x, c = coords()
    zh, zl = z // 2, lax.rem(z, 2)

    barrier = pltpu.get_barrier_semaphore()
    to_others(me, lambda i: pl.semaphore_signal(barrier, inc=1, device_id=(i,), device_id_type=MESH))

    def load_state(k, carry):
        def issue(which, rg, sub):
            for i, refs in enumerate(((w_attn, w_mlp, nw), (m_attn, m_mlp, nm), (v_attn, v_mlp, nv))):
                pltpu.make_async_copy(refs[which].at[pl.ds(rg * ROWS, ROWS), pl.ds(pl.multiple_of(sub * WIDTH, 128), WIDTH)], refs[2].at[k], load_sem.at[i]).start()
        bank_of(k, lambda rg, sub: issue(0, rg, sub), lambda rg, sub: issue(1, rg, sub))
        return carry
    lax.fori_loop(0, CHUNKS, load_state, 0)
    pack_grads(g_vec, g_wide, g_small, big, long)

    pl.semaphore_wait(barrier, GROUP - 1)

    def a_of(t):
        return x if t == 0 else y

    def b_of(t):
        return y if t == 0 else x

    def a_peer(t, da, dc):
        cc = flip(c, dc)
        return index_of(z, y, flip(x, da), cc) if t == 0 else index_of(z, flip(y, da), x, cc)

    def b_peer(t):
        return index_of(z, 1 - y, x, c) if t == 0 else index_of(z, y, 1 - x, c)

    low_peer = index_of(zh * 2 + 1 - zl, y, x, c)
    high_peer = index_of((1 - zh) * 2 + zl, y, x, c)

    def first_start(j, t):
        k = 2 * j + t

        def issue(grad, rg, sub, own):
            def body(b, carry):
                zz = lax.rem(b, 2) * 2 + b // 4
                bb = lax.rem(b // 2, 2)
                for da in range(2):
                    for dc in range(2):
                        aa, cc = flip(a_of(t), da), flip(c, dc)
                        owner = index_of(zz, bb, aa, cc) if t == 0 else index_of(zz, aa, bb, cc)
                        src = grad.at[0, pl.ds(rg * ROWS, ROWS), pl.ds(pl.multiple_of(owner * own + sub * WIDTH, 128), WIDTH)]
                        dst = land.at[k, (da * 2 + dc) * 8 + b]
                        if da == 0 and dc == 0:
                            pltpu.make_async_copy(src, dst, s1_recv.at[k]).start()
                        else:
                            remote(src, dst, s1_send.at[k], s1_recv.at[k], a_peer(t, da, dc)).start()
                return carry
            lax.fori_loop(0, 8, body, 0)
        bank_of(k, lambda rg, sub: issue(g_attn, rg, sub, OWN_A), lambda rg, sub: issue(g_mlp, rg, sub, OWN_M))

    def first_finish(j, t):
        k = 2 * j + t
        slot = lax.rem(j, SLOTS) * 2 + t

        @pl.when(j >= SLOTS)
        def _():
            wait_bytes(s2buf.at[k - 2 * SLOTS], s2_send.at[k - 2 * SLOTS])
        wait_bytes(land.at[k], s1_recv.at[k])

        def body(b, carry):
            for i in range(TILES):
                cols = pl.ds(i * 128, 128)
                parts = [land[k, p * 8 + b, :, cols].astype(F32) for p in range(4)]
                acc1[slot, b, :, cols] = (parts[0] + parts[1]) + (parts[2] + parts[3])
            return carry
        lax.fori_loop(0, 8, body, 0)
        remote(acc1.at[slot, pl.ds((1 - zl) * 4, 4)], s2buf.at[k], s2_send.at[k], s2_recv.at[k], low_peer).start()

    def second_finish(j, t):
        k = 2 * j + t
        slot = lax.rem(j, SLOTS) * 2 + t
        wait_bytes(s2buf.at[k], s2_recv.at[k])

        def body(b, carry):
            for i in range(TILES):
                cols = pl.ds(i * 128, 128)
                s2buf[k, b, :, cols] = s2buf[k, b, :, cols] + acc1[slot, zl * 4 + b, :, cols]
            return carry
        lax.fori_loop(0, 4, body, 0)
        remote(s2buf.at[k, pl.ds((1 - b_of(t)) * 2, 2)], s3buf.at[k], s3_send.at[k], s3_recv.at[k], b_peer(t)).start()

    def third_finish(j, t):
        k = 2 * j + t
        wait_bytes(s3buf.at[k], s3_recv.at[k])
        for b in range(2):
            for i in range(TILES):
                cols = pl.ds(i * 128, 128)
                s3buf[k, b, :, cols] = s3buf[k, b, :, cols] + s2buf[k, b_of(t) * 2 + b, :, cols]
        remote(s3buf.at[k, 1 - zh], s4buf.at[k], s4_send.at[k], s4_recv.at[k], high_peer).start()

    def fourth_finish(j, t):
        k = 2 * j + t
        wait_bytes(s4buf.at[k], s4_recv.at[k])
        total = n_acc[...]
        for i in range(TILES):
            cols = pl.ds(i * 128, 128)
            gs = (s3buf[k, zh, :, cols] + s4buf[k, :, cols]) * (1.0 / GROUP)
            gsum[k, :, cols] = gs
            total = total + gs * gs
        n_acc[...] = total

    for j in range(AHEAD):
        for t in range(2):
            first_start(j, t)

    def small_start(i):
        remote(g_small.at[i], small_in.at[me], misc_send.at[0], misc_recv.at[0], i).start()
    to_others(me, small_start)
    small_in[me] = g_small[me]

    for i, (vec_ref, wide_ref, fill) in enumerate(((w_vec, w_wide, 1.0), (m_vec, m_wide, 0.0), (v_vec, v_wide, 1.0))):
        state_small[i] = pack_state(vec_ref, wide_ref, flat, square, fill)
    for i, ref in enumerate((nw, nm, nv)):
        wait_bytes(ref, load_sem.at[i])
    n_acc[...] = jnp.zeros_like(n_acc)
    rows_w[...] = jnp.zeros_like(rows_w)
    rows_u[...] = jnp.zeros_like(rows_u)

    def weight_squares(k, carry):
        total = rows_w[row_group(k)]
        for i in range(TILES):
            w = nw[k, :, pl.ds(i * 128, 128)]
            total = total + w * w
        rows_w[row_group(k)] = total
        return carry
    lax.fori_loop(0, CHUNKS, weight_squares, 0)

    def pipeline(stages, first=None):
        def body(j, carry):
            if first is not None:
                @pl.when(j + AHEAD < PAIRS)
                def _():
                    for t in range(2):
                        first(j + AHEAD, t)
            for lag, stage in enumerate(stages):
                @pl.when(jnp.logical_and(j >= lag, j < PAIRS + lag))
                def _():
                    for t in range(2):
                        stage(j - lag, t)
            return carry
        lax.fori_loop(0, PAIRS + len(stages) - 1, body, 0)
    pipeline((first_finish, second_finish, third_finish, fourth_finish), first_start)

    wait_bytes(small_in.at[pl.ds(0, GROUP - 1)], misc_recv.at[0])
    wait_bytes(small_in.at[pl.ds(0, GROUP - 1)], misc_send.at[0])
    gs_small = jnp.sum(small_in[...], axis=0) * (1.0 / GROUP)

    sub_iota = lax.broadcasted_iota(jnp.int32, (4, 128), 0)
    eye = lax.broadcasted_iota(jnp.int32, (96, 128), 0) == lax.broadcasted_iota(jnp.int32, (96, 128), 1)

    def to_row(column_parts):
        sums = jnp.sum(column_parts, axis=1, keepdims=True)
        return jnp.sum(jnp.where(eye, jnp.broadcast_to(sums, (96, 128)), 0.0), axis=0, keepdims=True)

    def message(row0, small, row3):
        half = jnp.sum(small, axis=0, keepdims=True)
        return (jnp.where(sub_iota == 0, jnp.broadcast_to(row0, (4, 128)), 0.0)
                + jnp.where(sub_iota == 1, jnp.broadcast_to(half[:, :128], (4, 128)), 0.0)
                + jnp.where(sub_iota == 2, jnp.broadcast_to(half[:, 128:], (4, 128)), 0.0)
                + jnp.where(sub_iota == 3, jnp.broadcast_to(row3, (4, 128)), 0.0))

    def sum_over_devices(value, slot, inbox):
        msg[slot] = value
        inbox[me] = value

        def start(i):
            remote(msg.at[slot], inbox.at[me], misc_send.at[1 + slot], misc_recv.at[1 + slot], i).start()
        to_others(me, start)
        wait_bytes(inbox.at[pl.ds(0, GROUP - 1)], misc_recv.at[1 + slot])
        wait_bytes(inbox.at[pl.ds(0, GROUP - 1)], misc_send.at[1 + slot])
        return jnp.sum(inbox[...], axis=0)

    small_w = state_small[0]
    small_sq = gs_small * gs_small
    square_row = jnp.sum(n_acc[...], axis=0, keepdims=True) + jnp.sum(small_sq[:, :128], axis=0, keepdims=True) + jnp.sum(small_sq[:, 128:], axis=0, keepdims=True)
    first_sums = sum_over_devices(message(to_row(rows_w[...].reshape(96, 128)), small_w * small_w, square_row), 0, inbox1)
    clip = jnp.minimum(1.0, MAX_NORM / jnp.sqrt(jnp.sum(first_sums[3:4], axis=1, keepdims=True)))
    clip_tile[...] = jnp.broadcast_to(clip, (ROWS, 128))

    def direction(k, carry):
        cl = clip_tile[...]
        total = rows_u[row_group(k)]
        for i in range(TILES):
            cols = pl.ds(i * 128, 128)
            u, m1, v1 = adam(gsum[k, :, cols], nw[k, :, cols], nm[k, :, cols], nv[k, :, cols], cl)
            nm[k, :, cols] = m1
            nv[k, :, cols] = v1
            gsum[k, :, cols] = u
            total = total + u * u
        rows_u[row_group(k)] = total
        return carry
    lax.fori_loop(0, CHUNKS, direction, 0)
    u_small, m1_small, v1_small = adam(gs_small, small_w, state_small[1], state_small[2], jnp.broadcast_to(clip, (8, 256)))
    second_sums = sum_over_devices(message(to_row(rows_u[...].reshape(96, 128)), u_small * u_small, jnp.zeros((1, 128), F32)), 1, inbox2)

    ratio_row = jnp.sqrt(first_sums[0:1]) / jnp.sqrt(second_sums[0:1])
    ratio_col = jnp.sum(jnp.where(eye, jnp.broadcast_to(ratio_row, (96, 128)), 0.0), axis=1, keepdims=True)
    ratio[...] = jnp.broadcast_to(LEARN_RATE * ratio_col, (96, 128)).reshape(6, ROWS, 128)

    lane = lax.broadcasted_iota(jnp.int32, (1, 128), 1)

    def small_totals(sums):
        upper = sums[2:3]
        wide = jnp.where(lane >= 64, upper, 0.0)
        for shift in (64, 32, 16):
            wide = wide + pltpu.roll(wide, shift, 1)
        return sums[1:2], jnp.where(lane >= 64, wide, upper)

    def gather_high(j, t):
        k = 2 * j + t
        mine = a_of(t) * 16 + c * 8 + zl * 4 + b_of(t) * 2 + zh
        rr = ratio[row_group(k)]
        for i in range(TILES):
            cols = pl.ds(i * 128, 128)
            w1 = nw[k, :, cols] - rr * gsum[k, :, cols]
            nw[k, :, cols] = w1
            land[k, mine, :, cols] = w1.astype(BF16)
        part = land.at[k, mine]
        remote(part, part, s4_send.at[k], s4_recv.at[k], high_peer).start()

    def gather_b(j, t):
        k = 2 * j + t
        wait_bytes(land.at[k, 0], s4_recv.at[k])
        part = land.at[k, pl.ds(a_of(t) * 16 + c * 8 + zl * 4 + b_of(t) * 2, 2)]
        remote(part, part, s3_send.at[k], s3_recv.at[k], b_peer(t)).start()

    def gather_low(j, t):
        k = 2 * j + t
        wait_bytes(land.at[k, pl.ds(0, 2)], s3_recv.at[k])
        part = land.at[k, pl.ds(a_of(t) * 16 + c * 8 + zl * 4, 4)]
        remote(part, part, s2_send.at[k], s2_recv.at[k], low_peer).start()

    def gather_a(j, t):
        k = 2 * j + t
        wait_bytes(land.at[k, pl.ds(0, 4)], s2_recv.at[k])
        part = land.at[k, pl.ds(a_of(t) * 16 + c * 8, 8)]
        remote(part, part, s1_send.at[k], s1_recv.at[k], a_peer(t, 1, 0)).start()
        remote(part, part, d_send.at[k], d_recv.at[k], a_peer(t, 0, 1)).start()

    def gather_core(j, t):
        k = 2 * j + t
        wait_bytes(land.at[k, pl.ds(0, 8)], s1_recv.at[k])
        part = land.at[k, pl.ds((1 - a_of(t)) * 16 + c * 8, 8)]
        remote(part, part, d_send.at[k], d_recv.at[k], a_peer(t, 0, 1)).start()

    def drain_reduce(k, carry):
        wait_bytes(land.at[k, pl.ds(0, 24)], s1_send.at[k])

        @pl.when(k >= CHUNKS - 2 * SLOTS)
        def _():
            wait_bytes(s2buf.at[k], s2_send.at[k])
        wait_bytes(s3buf.at[k], s3_send.at[k])
        wait_bytes(s4buf.at[k], s4_send.at[k])
        return carry
    lax.fori_loop(0, CHUNKS, drain_reduce, 0)

    w_low, w_high = small_totals(first_sums)
    u_low, u_high = small_totals(second_sums)
    r_low = LEARN_RATE * (jnp.sqrt(w_low) / jnp.sqrt(u_low))
    r_high = LEARN_RATE * (jnp.sqrt(w_high) / jnp.sqrt(u_high))
    r_small = jnp.concatenate([jnp.broadcast_to(r_low, (8, 128)), jnp.broadcast_to(r_high, (8, 128))], axis=1)
    new_small = small_w - r_small * u_small
    small_new[...] = new_small
    small_all[me] = new_small
    state_small[1] = m1_small
    state_small[2] = v1_small

    def small_stage(j, t):
        if t == 1:
            return

        @pl.when(j == 0)
        def _():
            to_others(me, lambda i: remote(small_new, small_all.at[me], misc_send.at[3], misc_recv.at[3], i).start())
            unpack_state(small_new[...], nw_vec, nw_wide, square)
            unpack_state(state_small[1], nm_vec, nm_wide, square)
            unpack_state(state_small[2], nv_vec, nv_wide, square)

        @pl.when(j == PAIRS - 3)
        def _():
            wait_bytes(small_all.at[pl.ds(0, GROUP - 1)], misc_recv.at[3])
            wait_bytes(small_all.at[pl.ds(0, GROUP - 1)], misc_send.at[3])
            unpack_replica(small_all, rep_vec, rep_wide)
    pipeline((gather_high, gather_b, gather_low, gather_a, gather_core, small_stage))

    def drain_gather(k, carry):
        wait_bytes(land.at[k, pl.ds(0, 16)], d_recv.at[k])
        wait_bytes(land.at[k, pl.ds(0, 16)], d_send.at[k])
        wait_bytes(land.at[k, pl.ds(0, 8)], s1_send.at[k])
        wait_bytes(land.at[k, pl.ds(0, 4)], s2_send.at[k])
        wait_bytes(land.at[k, pl.ds(0, 2)], s3_send.at[k])
        wait_bytes(land.at[k, 0], s4_send.at[k])
        return carry
    lax.fori_loop(0, CHUNKS, drain_gather, 0)


def store_kernel(land, nw, nm, nv, *refs):
    small, (rep_attn, rep_mlp, w_attn, w_mlp, m_attn, m_mlp, v_attn, v_mlp), small_out, sem = refs[:8], refs[8:16], refs[16:24], refs[24]
    state_out = ((nw, w_attn, w_mlp), (nm, m_attn, m_mlp), (nv, v_attn, v_mlp))
    for i in range(8):
        pltpu.make_async_copy(small[i], small_out[i], sem.at[4 + i]).start()

    def pair_body(j, carry):
        for t in range(2):
            k = 2 * j + t

            def issue(rep, which, own, rg, sub):
                rows = pl.ds(pl.multiple_of(rg * ROWS, ROWS), ROWS)
                base = sub * WIDTH
                for q in range(32):
                    aa, cc, zl, bb, zh = q // 16, q // 8 % 2, q // 4 % 2, q // 2 % 2, q % 2
                    owner = index_of(zh * 2 + zl, bb, aa, cc) if t == 0 else index_of(zh * 2 + zl, aa, bb, cc)
                    pltpu.make_async_copy(land.at[k, q], rep.at[rows, pl.ds(pl.multiple_of(base + owner * own, 128), WIDTH)], sem.at[0]).start()
                for i, refs in enumerate(state_out):
                    pltpu.make_async_copy(refs[0].at[k], refs[1 + which].at[rows, pl.ds(pl.multiple_of(base, 128), WIDTH)], sem.at[1 + i]).start()
            bank_of(k, lambda rg, sub: issue(rep_attn, 0, OWN_A, rg, sub), lambda rg, sub: issue(rep_mlp, 1, OWN_M, rg, sub))
        return carry
    lax.fori_loop(0, PAIRS, pair_body, 0)
    wait_bytes(land, sem.at[0])
    for i, refs in enumerate(state_out):
        wait_bytes(refs[0], sem.at[1 + i])
    for i in range(8):
        pltpu.make_async_copy(small[i], small_out[i], sem.at[4 + i]).wait()


def solution(mesh):
    grad_spec = P(AXIS, None, None)
    shard_spec = P(None, AXIS)
    full_spec = P(None, None)

    def local_step(g_attn, g_mlp, g_wide, g_vec, w_attn, w_mlp, w_wide, w_vec, m_attn, m_mlp, m_wide, m_vec, v_attn, v_mlp, v_wide, v_vec):
        hbm = pl.BlockSpec(memory_space=pl.ANY)
        vmem = pl.BlockSpec(memory_space=pltpu.VMEM)
        block = (CHUNKS, ROWS, WIDTH)
        small_shapes = [((146, 256), BF16), ((16, 1024), BF16)] + [((8, 146), F32), ((16, 32), F32)] * 3
        dma = pltpu.SemaphoreType.DMA
        land, nw, nm, nv, *small = pl.pallas_call(
            step_kernel,
            out_shape=[pltpu.VMEM((CHUNKS, 32, ROWS, WIDTH), BF16), pltpu.VMEM(block, F32), pltpu.VMEM(block, F32), pltpu.VMEM(block, F32)]
            + [pltpu.VMEM(shape, dtype) for shape, dtype in small_shapes],
            in_specs=[hbm, hbm, vmem, vmem] + [hbm] * 6 + [vmem] * 6,
            out_specs=[vmem] * 12,
            scratch_shapes=[
                pltpu.VMEM((2 * SLOTS, 8, ROWS, WIDTH), F32),
                pltpu.VMEM((CHUNKS, 4, ROWS, WIDTH), F32),
                pltpu.VMEM((CHUNKS, 2, ROWS, WIDTH), F32),
                pltpu.VMEM(block, F32),
                pltpu.VMEM(block, F32),
                pltpu.VMEM((GROUP, 8, 256), F32),
                pltpu.VMEM((GROUP, 8, 256), F32),
                pltpu.VMEM((GROUP, 8, 256), F32),
                pltpu.VMEM((8, 256), F32),
                pltpu.VMEM((3, 8, 256), F32),
                pltpu.VMEM((256, 256), F32),
                pltpu.VMEM((128, 1024), F32),
                pltpu.VMEM((8, 256), F32),
                pltpu.VMEM((128, 128), F32),
                pltpu.VMEM((2, 4, 128), F32),
                pltpu.VMEM((GROUP, 4, 128), F32),
                pltpu.VMEM((GROUP, 4, 128), F32),
                pltpu.VMEM((6, ROWS, 128), F32),
                pltpu.VMEM((6, ROWS, 128), F32),
                pltpu.VMEM((6, ROWS, 128), F32),
                pltpu.VMEM((ROWS, 128), F32),
                pltpu.VMEM((ROWS, 128), F32),
            ] + [dma((CHUNKS,))] * 10 + [dma((3,)), dma((4,)), dma((4,))],
            compiler_params=pltpu.CompilerParams(collective_id=0, has_side_effects=True, vmem_limit_bytes=30 * 1024 * 1024),
            name="lamb_step",
        )(g_attn, g_mlp, g_vec, g_wide, w_attn, w_mlp, m_attn, m_mlp, v_attn, v_mlp, w_vec.T, w_wide, m_vec.T, m_wide, v_vec.T, v_wide)
        shard_a = jax.ShapeDtypeStruct((64, OWN_A), F32)
        shard_m = jax.ShapeDtypeStruct((32, OWN_M), F32)
        (rep_attn, rep_mlp, nw_attn, nw_mlp, nm_attn, nm_mlp, nv_attn, nv_mlp,
         rep_vec, rep_wide, nw_vec, nw_wide, nm_vec, nm_wide, nv_vec, nv_wide) = pl.pallas_call(
            store_kernel,
            out_shape=[jax.ShapeDtypeStruct((64, OWN_A * GROUP), BF16), jax.ShapeDtypeStruct((32, OWN_M * GROUP), BF16),
                       shard_a, shard_m, shard_a, shard_m, shard_a, shard_m] + [jax.ShapeDtypeStruct(shape, dtype) for shape, dtype in small_shapes],
            in_specs=[vmem] * 12,
            out_specs=[hbm] * 16,
            scratch_shapes=[dma((12,))],
            compiler_params=pltpu.CompilerParams(vmem_limit_bytes=1024 * 1024),
            name="store_results",
        )(land, nw, nm, nv, *small)
        return (rep_attn, rep_mlp, rep_wide, rep_vec, nw_attn, nw_mlp, nw_wide, nw_vec.T, nm_attn, nm_mlp, nm_wide, nm_vec.T, nv_attn, nv_mlp, nv_wide, nv_vec.T)

    return jax.shard_map(local_step, mesh=mesh, in_specs=(grad_spec,) * 4 + (shard_spec,) * 12, out_specs=(full_spec,) * 4 + (shard_spec,) * 12, check_vma=False)
```

```python
import jax
import jax.numpy as jnp
from jax import lax
from jax.experimental import pallas as pl
from jax.experimental.pallas import tpu as pltpu
from jax.sharding import PartitionSpec as P

STEP_NUMBER = 10
LEARN_RATE = 0.04
BETA_FIRST = 0.9
BETA_SECOND = 0.999
EPSILON = 1e-6
WEIGHT_DECAY = 0.01
MAX_NORM = 1.0
FIRST_SCALE = 1.0 / (1.0 - BETA_FIRST ** STEP_NUMBER)
SECOND_SCALE = 1.0 / (1.0 - BETA_SECOND ** STEP_NUMBER)

AXIS = "data"
MESH = pl.DeviceIdType.MESH
F32 = jnp.float32
BF16 = jnp.bfloat16
LANES = 128
SUBLANES = 8
MIB = 1024 * 1024

GROUP = 32
ROWS = 16
WIDTH = 512
OWN_A = 2048
OWN_M = 8192
SUB_A = OWN_A // WIDTH
SUB_M = OWN_M // WIDTH
CHUNKS_A = 4 * SUB_A
CHUNKS = CHUNKS_A + 2 * SUB_M
PAIRS = CHUNKS // 2
GROUPS = 6
ROW_COUNT = GROUPS * ROWS
AHEAD = 1
SLOTS = 3
TAIL = 2
HEAD = 2
REDUCE_LAGS = (0, 1, 2, 3)
GATHER_LAGS = (0, 1, 2, 3, 4, 5)
VEC_ROWS = 146
WIDE_ROWS = 16
WIDE_LANE = 64
WIDE_COLS = 32

WEIGHT = {"h": 16, "l": 8, "y": 4, "x": 2, "c": 1}
PLAIN = (("x", "l", "y"), ("y", "l", "x"))
SWAPPED = (("x", "y", "l"), ("y", "x", "l"))


def own_bits():
    me = lax.axis_index(AXIS)
    return me, {name: lax.rem(me // weight, 2) for name, weight in WEIGHT.items()}


def index_of(**bits):
    return sum(bits[name] * weight for name, weight in WEIGHT.items())


def flip(bit, other):
    return bit + other - 2 * bit * other


def remote(src, dst, send_sem, recv_sem, device):
    return pltpu.make_async_remote_copy(src_ref=src, dst_ref=dst, send_sem=send_sem, recv_sem=recv_sem, device_id=(device,), device_id_type=MESH)


def wait_bytes(ref, sem):
    pltpu.make_async_copy(ref, ref, sem).wait()


def loop(count, body, **kw):
    def step(i, carry):
        body(i)
        return carry
    lax.fori_loop(0, count, step, 0, **kw)


def tiles():
    return [pl.ds(i * LANES, LANES) for i in range(WIDTH // LANES)]


def clear(ref):
    ref[:] = jnp.zeros_like(ref)


def bank_of(k, issue):
    @pl.when(k < CHUNKS_A)
    def _():
        issue("attn", OWN_A, k // SUB_A, lax.rem(k, SUB_A))

    @pl.when(k >= CHUNKS_A)
    def _():
        local = k - CHUNKS_A
        issue("mlp", OWN_M, local // SUB_M, lax.rem(local, SUB_M))


def row_group(k):
    return jnp.where(k < CHUNKS_A, k // SUB_A, CHUNKS_A // SUB_A + (k - CHUNKS_A) // SUB_M)


def block_at(ref, rg, column):
    return ref.at[pl.ds(pl.multiple_of(rg * ROWS, ROWS), ROWS), pl.ds(pl.multiple_of(column, LANES), WIDTH)]


def adam(gs, w, m, v, clip):
    clipped = clip * gs
    new_m = BETA_FIRST * m + (1.0 - BETA_FIRST) * clipped
    new_v = BETA_SECOND * v + (1.0 - BETA_SECOND) * (clipped * clipped)
    u = (new_m * FIRST_SCALE) / (jnp.sqrt(new_v * SECOND_SCALE) + EPSILON) + WEIGHT_DECAY * w
    return u, new_m, new_v


def to_others(me, start_one):
    loop(GROUP - 1, lambda i: start_one(lax.rem(me + 1 + i, GROUP)))


def wide_shift(g):
    return WIDE_LANE + WIDE_ROWS * g


def wide_back(g):
    return (LANES - wide_shift(g)) % LANES


def rolled(x, shift):
    return pltpu.roll(x, shift, 1) if shift else x


def pack_state(vec_ref, wide_ref, flat, square, fill):
    clear(flat)
    flat[:, :VEC_ROWS] = vec_ref[:]
    clear(square)
    square[:WIDE_ROWS, :WIDE_COLS] = wide_ref[:]
    wide_t = square[:].T
    wide = sum(rolled(wide_t[SUBLANES * g:SUBLANES * (g + 1)], wide_shift(g)) for g in range(4))
    vec = flat[:]
    lane = lax.broadcasted_iota(jnp.int32, vec.shape, 1)
    packed = jnp.concatenate([vec[:, :LANES], vec[:, LANES:] + wide], axis=1)
    return jnp.where(jnp.logical_and(lane >= VEC_ROWS, lane < LANES + WIDE_LANE), fill, packed)


def unpack_state(packed, vec_ref, wide_ref, square):
    vec_ref[:] = packed[:, :VEC_ROWS]
    clear(square)
    for g in range(4):
        square[SUBLANES * g:SUBLANES * (g + 1), :] = rolled(packed[:, LANES:], wide_back(g))
    wide_ref[:] = square[:].T[:WIDE_ROWS, :WIDE_COLS]


def pack_grads(g_vec, g_wide, g_small, big, long):
    clear(big)
    big[:VEC_ROWS, :] = g_vec[0].astype(F32)
    clear(long)
    long[:WIDE_ROWS, :] = g_wide[0].astype(F32)
    vec = big[:].T
    wide_t = long[:].T.reshape(GROUP, 4, SUBLANES, LANES)
    wide = sum(rolled(wide_t[:, g].reshape(GROUP * SUBLANES, LANES), wide_shift(g)) for g in range(4))
    g_small[:, :, :LANES] = vec[:, :LANES].reshape(GROUP, SUBLANES, LANES).astype(BF16)
    g_small[:, :, LANES:] = (vec[:, LANES:] + wide).reshape(GROUP, SUBLANES, LANES).astype(BF16)


def unpack_replica(small_all, rep_vec, rep_wide):
    rep_vec[:] = small_all[:].astype(F32).reshape(GROUP * SUBLANES, 2 * LANES).T[:VEC_ROWS].astype(BF16)
    upper = small_all[:, :, LANES:].astype(F32).reshape(GROUP * SUBLANES, LANES)
    parts = [rolled(upper, wide_back(g)).reshape(GROUP, 1, SUBLANES, LANES) for g in range(4)]
    rep_wide[:] = jnp.concatenate(parts, axis=1).reshape(GROUP * WIDE_COLS, LANES).T[:WIDE_ROWS].astype(BF16)


def step_kernel(g_attn, g_mlp, g_vec, g_wide, w_attn, w_mlp, m_attn, m_mlp, v_attn, v_mlp, w_vec, w_wide, m_vec, m_wide, v_vec, v_wide,
                land, nw, nm, nv, rep_vec, rep_wide, nw_vec, nw_wide, nm_vec, nm_wide, nv_vec, nv_wide,
                acc1, s2buf, s3buf, s4buf, gsum, g_small, small_in, small_all, small_new, state_small, big, long, flat, square,
                msg, inboxes, rows_w, rows_u, ratio, clip_tile, n_acc,
                s1_send, s1_recv, s2_send, s2_recv, s3_send, s3_recv, s4_send, s4_recv, d_send, d_recv, load_sem, misc_send, misc_recv):
    me, bits = own_bits()
    grads = {"attn": g_attn, "mlp": g_mlp}
    states = {"attn": (w_attn, m_attn, v_attn), "mlp": (w_mlp, m_mlp, v_mlp)}

    def peer(name):
        return index_of(**{**bits, name: 1 - bits[name]})

    barrier = pltpu.get_barrier_semaphore()
    to_others(me, lambda i: pl.semaphore_signal(barrier, inc=1, device_id=(i,), device_id_type=MESH))

    def load_state(k):
        def issue(bank, own, rg, sub):
            for i, dst in enumerate((nw, nm, nv)):
                pltpu.make_async_copy(block_at(states[bank][i], rg, sub * WIDTH), dst.at[k], load_sem.at[i]).start()
        bank_of(k, issue)
    loop(CHUNKS, load_state)
    pack_grads(g_vec, g_wide, g_small, big, long)

    pl.semaphore_wait(barrier, GROUP - 1)

    def first_start(j, t, order):
        k = 2 * j + t
        one, two, three = order

        def issue(bank, own, rg, sub):
            def body(b):
                for da in range(2):
                    for dc in range(2):
                        target = {one: flip(bits[one], da), "c": flip(bits["c"], dc)}
                        owner = index_of(**target, **{two: b // 4, three: lax.rem(b // 2, 2), "h": lax.rem(b, 2)})
                        src = block_at(grads[bank].at[0], rg, owner * own + sub * WIDTH)
                        dst = land.at[k, (da * 2 + dc) * 8 + b]
                        if da or dc:
                            remote(src, dst, s1_send.at[k], s1_recv.at[k], index_of(**{**bits, **target})).start()
                        else:
                            pltpu.make_async_copy(src, dst, s1_recv.at[k]).start()
            loop(8, body)
        bank_of(k, issue)

    def first_finish(j, t, order):
        k = 2 * j + t
        slot = lax.rem(j, SLOTS) * 2 + t

        @pl.when(j >= SLOTS)
        def _():
            wait_bytes(s2buf.at[k - 2 * SLOTS], s2_send.at[k - 2 * SLOTS])
        wait_bytes(land.at[k], s1_recv.at[k])

        def body(b):
            for cols in tiles():
                own, core, far, both = [land[k, p * 8 + b, :, cols].astype(F32) for p in range(4)]
                acc1[slot, b, :, cols] = (own + core) + (far + both)
        loop(8, body)
        remote(acc1.at[slot, pl.ds((1 - bits[order[1]]) * 4, 4)], s2buf.at[k], s2_send.at[k], s2_recv.at[k], peer(order[1])).start()

    def second_finish(j, t, order):
        k = 2 * j + t
        slot = lax.rem(j, SLOTS) * 2 + t
        two, three = bits[order[1]], bits[order[2]]
        wait_bytes(s2buf.at[k], s2_recv.at[k])

        def body(b):
            for cols in tiles():
                s2buf[k, b, :, cols] = s2buf[k, b, :, cols] + acc1[slot, two * 4 + b, :, cols]
        loop(4, body)
        remote(s2buf.at[k, pl.ds((1 - three) * 2, 2)], s3buf.at[k], s3_send.at[k], s3_recv.at[k], peer(order[2])).start()

    def third_finish(j, t, order):
        k = 2 * j + t
        wait_bytes(s3buf.at[k], s3_recv.at[k])
        for b in range(2):
            for cols in tiles():
                s3buf[k, b, :, cols] = s3buf[k, b, :, cols] + s2buf[k, bits[order[2]] * 2 + b, :, cols]
        remote(s3buf.at[k, 1 - bits["h"]], s4buf.at[k], s4_send.at[k], s4_recv.at[k], peer("h")).start()

    def fourth_finish(j, t, order):
        k = 2 * j + t
        wait_bytes(s4buf.at[k], s4_recv.at[k])
        total = n_acc[:]
        for cols in tiles():
            gs = (s3buf[k, bits["h"], :, cols] + s4buf[k, :, cols]) * (1.0 / GROUP)
            gsum[k, :, cols] = gs
            total = total + gs * gs
        n_acc[:] = total

    def pair(stage, j, plain):
        for orders, chosen in ((PLAIN, plain), (SWAPPED, jnp.logical_not(plain))):
            @pl.when(chosen)
            def _():
                for t, order in enumerate(orders):
                    stage(j, t, order)

    for j in range(AHEAD):
        for t, order in enumerate(PLAIN):
            first_start(j, t, order)

    to_others(me, lambda i: remote(g_small.at[i], small_in.at[me], misc_send.at[0], misc_recv.at[0], i).start())
    small_in[me] = g_small[me]

    for i, (vec_ref, wide_ref, fill) in enumerate(((w_vec, w_wide, 1.0), (m_vec, m_wide, 0.0), (v_vec, v_wide, 1.0))):
        state_small[i] = pack_state(vec_ref, wide_ref, flat, square, fill)
    for i, ref in enumerate((nw, nm, nv)):
        wait_bytes(ref, load_sem.at[i])
    clear(n_acc)
    clear(rows_w)
    clear(rows_u)

    def weight_squares(k):
        total = rows_w[row_group(k)]
        for cols in tiles():
            w = nw[k, :, cols]
            total = total + w * w
        rows_w[row_group(k)] = total
    loop(CHUNKS, weight_squares)

    def reduce_step(j):
        @pl.when(j + AHEAD < PAIRS)
        def _():
            pair(first_start, j + AHEAD, j + AHEAD < PAIRS - TAIL)
        for lag, stage in zip(REDUCE_LAGS, (first_finish, second_finish, third_finish, fourth_finish)):
            @pl.when(jnp.logical_and(j >= lag, j < PAIRS + lag))
            def _():
                pair(stage, j - lag, j - lag < PAIRS - TAIL)
    loop(PAIRS + max(REDUCE_LAGS), reduce_step)

    wait_bytes(small_in.at[:GROUP - 1], misc_recv.at[0])
    wait_bytes(small_in.at[:GROUP - 1], misc_send.at[0])
    gs_small = jnp.sum(small_in[:].astype(F32), axis=0) * (1.0 / GROUP)

    sub_iota = lax.broadcasted_iota(jnp.int32, msg.shape[1:], 0)
    square_shape = (ROW_COUNT, LANES)
    eye = lax.broadcasted_iota(jnp.int32, square_shape, 0) == lax.broadcasted_iota(jnp.int32, square_shape, 1)

    def to_row(column_parts):
        sums = jnp.sum(column_parts, axis=1, keepdims=True)
        return jnp.sum(jnp.where(eye, jnp.broadcast_to(sums, square_shape), 0.0), axis=0, keepdims=True)

    def halves(small):
        sums = jnp.sum(small, axis=0, keepdims=True)
        return sums[:, :LANES], sums[:, LANES:]

    def sum_over_devices(rows, slot):
        inbox = inboxes.at[slot]
        value = sum(jnp.where(sub_iota == i, jnp.broadcast_to(row, sub_iota.shape), 0.0) for i, row in enumerate(rows))
        msg[slot] = value
        inbox[me] = value
        to_others(me, lambda i: remote(msg.at[slot], inbox.at[me], misc_send.at[1 + slot], misc_recv.at[1 + slot], i).start())
        wait_bytes(inbox.at[:GROUP - 1], misc_recv.at[1 + slot])
        wait_bytes(inbox.at[:GROUP - 1], misc_send.at[1 + slot])
        total = jnp.sum(inbox[:], axis=0)
        return [total[i:i + 1] for i in range(4)]

    small_w = state_small[0]
    low, high = halves(gs_small * gs_small)
    square_row = jnp.sum(n_acc[:], axis=0, keepdims=True) + low + high
    w_large, w_low, w_high, squares = sum_over_devices((to_row(rows_w[:].reshape(square_shape)), *halves(small_w * small_w), square_row), 0)
    clip = jnp.minimum(1.0, MAX_NORM / jnp.sqrt(jnp.sum(squares, axis=1, keepdims=True)))
    clip_tile[:] = jnp.broadcast_to(clip, clip_tile.shape)

    def direction(k):
        cl = clip_tile[:]
        total = rows_u[row_group(k)]
        for cols in tiles():
            u, m1, v1 = adam(gsum[k, :, cols], nw[k, :, cols], nm[k, :, cols], nv[k, :, cols], cl)
            nm[k, :, cols] = m1
            nv[k, :, cols] = v1
            gsum[k, :, cols] = u
            total = total + u * u
        rows_u[row_group(k)] = total
    loop(CHUNKS, direction)
    u_small, m1_small, v1_small = adam(gs_small, small_w, state_small[1], state_small[2], jnp.broadcast_to(clip, small_w.shape))
    u_large, u_low, u_high, _ = sum_over_devices((to_row(rows_u[:].reshape(square_shape)), *halves(u_small * u_small)), 1)

    ratio_row = jnp.sqrt(w_large) / jnp.sqrt(u_large)
    ratio_col = jnp.sum(jnp.where(eye, jnp.broadcast_to(ratio_row, square_shape), 0.0), axis=1, keepdims=True)
    ratio[:] = jnp.broadcast_to(LEARN_RATE * ratio_col, square_shape).reshape(ratio.shape)

    lane = lax.broadcasted_iota(jnp.int32, (1, LANES), 1)

    def small_ratio(w_sums, u_sums):
        return jnp.broadcast_to(LEARN_RATE * (jnp.sqrt(w_sums) / jnp.sqrt(u_sums)), (SUBLANES, LANES))

    def with_wide_totals(upper):
        wide = jnp.where(lane >= WIDE_LANE, upper, 0.0)
        for shift in (64, 32, 16):
            wide = wide + rolled(wide, shift)
        return jnp.where(lane >= WIDE_LANE, wide, upper)

    def span(k, order, depth):
        names = (order[0], "c", order[1], order[2], "h")[:depth]
        size = GROUP >> depth
        start = sum(bits[name] * (GROUP >> (i + 1)) for i, name in enumerate(names))
        return land.at[k, pl.ds(start, size)]

    def gather_high(j, t, order):
        k = 2 * j + t
        mine = span(k, order, 5)
        rr = ratio[row_group(k)]
        for cols in tiles():
            w1 = nw[k, :, cols] - rr * gsum[k, :, cols]
            nw[k, :, cols] = w1
            mine[0, :, cols] = w1.astype(BF16)
        remote(mine, mine, s4_send.at[k], s4_recv.at[k], peer("h")).start()

    def gather_three(j, t, order):
        k = 2 * j + t
        wait_bytes(land.at[k, :1], s4_recv.at[k])
        part = span(k, order, 4)
        remote(part, part, s3_send.at[k], s3_recv.at[k], peer(order[2])).start()

    def gather_two(j, t, order):
        k = 2 * j + t
        wait_bytes(land.at[k, :2], s3_recv.at[k])
        part = span(k, order, 3)
        remote(part, part, s2_send.at[k], s2_recv.at[k], peer(order[1])).start()

    def gather_one(j, t, order):
        k = 2 * j + t
        wait_bytes(land.at[k, :4], s2_recv.at[k])
        part = span(k, order, 2)
        remote(part, part, s1_send.at[k], s1_recv.at[k], peer(order[0])).start()
        remote(part, part, d_send.at[k], d_recv.at[k], peer("c")).start()

    def gather_core(j, t, order):
        k = 2 * j + t
        wait_bytes(land.at[k, :8], s1_recv.at[k])
        part = land.at[k, pl.ds((1 - bits[order[0]]) * 16 + bits["c"] * 8, 8)]
        remote(part, part, d_send.at[k], d_recv.at[k], peer("c")).start()

    def drain_reduce(k):
        wait_bytes(land.at[k, :24], s1_send.at[k])

        @pl.when(k >= CHUNKS - 2 * SLOTS)
        def _():
            wait_bytes(s2buf.at[k], s2_send.at[k])
        wait_bytes(s3buf.at[k], s3_send.at[k])
        wait_bytes(s4buf.at[k], s4_send.at[k])
    loop(CHUNKS, drain_reduce)

    r_small = jnp.concatenate([small_ratio(w_low, u_low), small_ratio(with_wide_totals(w_high), with_wide_totals(u_high))], axis=1)
    state_small[0] = small_w - r_small * u_small
    state_small[1] = m1_small
    state_small[2] = v1_small
    small_new[:] = state_small[0].astype(BF16)
    small_all[me] = small_new[:]

    def gather_step(j):
        for lag, stage in zip(GATHER_LAGS, (gather_high, gather_three, gather_two, gather_one, gather_core)):
            @pl.when(jnp.logical_and(j >= lag, j < PAIRS + lag))
            def _():
                pair(stage, j - lag, j - lag >= HEAD)

        @pl.when(j == 4)
        def _():
            to_others(me, lambda i: remote(small_new, small_all.at[me], misc_send.at[3], misc_recv.at[3], i).start())
            for i, refs in enumerate(((nw_vec, nw_wide), (nm_vec, nm_wide), (nv_vec, nv_wide))):
                unpack_state(state_small[i], *refs, square)

        @pl.when(j == PAIRS)
        def _():
            wait_bytes(small_all.at[:GROUP - 1], misc_recv.at[3])
            wait_bytes(small_all.at[:GROUP - 1], misc_send.at[3])
            unpack_replica(small_all, rep_vec, rep_wide)
    loop(PAIRS + max(GATHER_LAGS), gather_step)

    def drain_gather(k):
        for size, sem in ((16, d_recv), (16, d_send), (8, s1_send), (4, s2_send), (2, s3_send), (1, s4_send)):
            wait_bytes(land.at[k, :size], sem.at[k])
    loop(CHUNKS, drain_gather)


def store_kernel(land, nw, nm, nv, *refs):
    small, large_out, small_out, sem = refs[:8], refs[8:16], refs[16:24], refs[24]
    outs = {"attn": large_out[::2], "mlp": large_out[1::2]}
    for i in range(8):
        pltpu.make_async_copy(small[i], small_out[i], sem.at[4 + i]).start()

    def store_pair(j, orders):
        for t, order in enumerate(orders):
            k = 2 * j + t

            def issue(bank, own, rg, sub):
                base = sub * WIDTH
                for q in range(GROUP):
                    names = (order[0], "c", order[1], order[2], "h")
                    owner = index_of(**{name: q * (2 << i) // GROUP % 2 for i, name in enumerate(names)})
                    pltpu.make_async_copy(land.at[k, q], block_at(outs[bank][0], rg, base + owner * own), sem.at[0]).start()
                for i, ref in enumerate((nw, nm, nv)):
                    pltpu.make_async_copy(ref.at[k], block_at(outs[bank][1 + i], rg, base), sem.at[1 + i]).start()
            bank_of(k, issue)
    loop(HEAD, lambda j: store_pair(j, SWAPPED))
    loop(PAIRS - HEAD, lambda j: store_pair(j + HEAD, PLAIN))
    wait_bytes(land, sem.at[0])
    for i, ref in enumerate((nw, nm, nv)):
        wait_bytes(ref, sem.at[1 + i])
    for i in range(8):
        pltpu.make_async_copy(small[i], small_out[i], sem.at[4 + i]).wait()


def solution(mesh):
    grad_spec = P(AXIS, None, None)
    shard_spec = P(None, AXIS)
    full_spec = P(None, None)
    hbm = pl.BlockSpec(memory_space=pl.ANY)
    in_vmem = pl.BlockSpec(memory_space=pltpu.VMEM)
    vmem, dma = pltpu.VMEM, pltpu.SemaphoreType.DMA
    block = (CHUNKS, ROWS, WIDTH)
    packed = (SUBLANES, 2 * LANES)
    small_shapes = [((VEC_ROWS, OWN_M // GROUP), BF16), ((WIDE_ROWS, WIDE_COLS * GROUP), BF16)] + [((SUBLANES, VEC_ROWS), F32), ((WIDE_ROWS, WIDE_COLS), F32)] * 3

    def local_step(g_attn, g_mlp, g_wide, g_vec, w_attn, w_mlp, w_wide, w_vec, m_attn, m_mlp, m_wide, m_vec, v_attn, v_mlp, v_wide, v_vec):
        scratch = [vmem((2 * SLOTS, 8, ROWS, WIDTH), F32), vmem((CHUNKS, 4, ROWS, WIDTH), F32), vmem((CHUNKS, 2, ROWS, WIDTH), F32), vmem(block, F32), vmem(block, F32)]
        scratch += [vmem((GROUP, *packed), BF16)] * 3 + [vmem(packed, BF16), vmem((3, *packed), F32)]
        scratch += [vmem((2 * LANES, GROUP * SUBLANES), F32), vmem((LANES, GROUP * WIDE_COLS), F32), vmem(packed, F32), vmem((LANES, LANES), F32)]
        scratch += [vmem((2, 4, LANES), F32), vmem((2, GROUP, 4, LANES), F32)] + [vmem((GROUPS, ROWS, LANES), F32)] * 3 + [vmem((ROWS, LANES), F32)] * 2
        scratch += [dma((CHUNKS,))] * 10 + [dma((3,)), dma((4,)), dma((4,))]
        results = pl.pallas_call(
            step_kernel,
            out_shape=[vmem((CHUNKS, GROUP, ROWS, WIDTH), BF16)] + [vmem(block, F32)] * 3 + [vmem(*item) for item in small_shapes],
            in_specs=[hbm] * 2 + [in_vmem] * 2 + [hbm] * 6 + [in_vmem] * 6,
            out_specs=[in_vmem] * 12,
            scratch_shapes=scratch,
            compiler_params=pltpu.CompilerParams(collective_id=0, has_side_effects=True, vmem_limit_bytes=30 * MIB),
            name="lamb_step",
        )(g_attn, g_mlp, g_vec, g_wide, w_attn, w_mlp, m_attn, m_mlp, v_attn, v_mlp, w_vec.T, w_wide, m_vec.T, m_wide, v_vec.T, v_wide)
        shards = [jax.ShapeDtypeStruct(w_attn.shape, F32), jax.ShapeDtypeStruct(w_mlp.shape, F32)] * 3
        (rep_attn, rep_mlp, nw_attn, nw_mlp, nm_attn, nm_mlp, nv_attn, nv_mlp,
         rep_vec, rep_wide, nw_vec, nw_wide, nm_vec, nm_wide, nv_vec, nv_wide) = pl.pallas_call(
            store_kernel,
            out_shape=[jax.ShapeDtypeStruct(g_attn.shape[1:], BF16), jax.ShapeDtypeStruct(g_mlp.shape[1:], BF16)] + shards + [jax.ShapeDtypeStruct(*item) for item in small_shapes],
            in_specs=[in_vmem] * 12,
            out_specs=[hbm] * 16,
            scratch_shapes=[dma((12,))],
            compiler_params=pltpu.CompilerParams(vmem_limit_bytes=MIB),
            name="store_results",
        )(*results)
        return (rep_attn, rep_mlp, rep_wide, rep_vec, nw_attn, nw_mlp, nw_wide, nw_vec.T, nm_attn, nm_mlp, nm_wide, nm_vec.T, nv_attn, nv_mlp, nv_wide, nv_vec.T)

    return jax.shard_map(local_step, mesh=mesh, in_specs=(grad_spec,) * 4 + (shard_spec,) * 12, out_specs=(full_spec,) * 4 + (shard_spec,) * 12, check_vma=False)
```

```python
import jax
import jax.numpy as jnp
from jax import lax
from jax.experimental import pallas as pl
from jax.experimental.pallas import tpu as pltpu
from jax.sharding import PartitionSpec as P

STEP_NUMBER = 10
LEARN_RATE = 0.04
BETA_FIRST = 0.9
BETA_SECOND = 0.999
EPSILON = 1e-6
WEIGHT_DECAY = 0.01
MAX_NORM = 1.0
FIRST_SCALE = 1.0 / (1.0 - BETA_FIRST ** STEP_NUMBER)
SECOND_SCALE = 1.0 / (1.0 - BETA_SECOND ** STEP_NUMBER)

AXIS = "data"
MESH = pl.DeviceIdType.MESH
F32 = jnp.float32
BF16 = jnp.bfloat16
LANES = 128
SUBLANES = 8
MIB = 1024 * 1024

GROUP = 32
ROWS = 16
WIDTH = 512
OWN_A = 2048
OWN_M = 8192
SUB_A = OWN_A // WIDTH
SUB_M = OWN_M // WIDTH
CHUNKS_A = 4 * SUB_A
CHUNKS = CHUNKS_A + 2 * SUB_M
PAIRS = CHUNKS // 2
GROUPS = 6
ROW_COUNT = GROUPS * ROWS
AHEAD = 1
SLOTS = 3
TAIL = 1
HEAD = 1
REDUCE_LAGS = (0, 1, 2, 3, 4)
GATHER_LAGS = (0, 1, 3, 5, 8, 9)
VEC_ROWS = 146
WIDE_ROWS = 16
WIDE_LANE = 64
WIDE_COLS = 32

WEIGHT = {"h": 16, "l": 8, "y": 4, "x": 2, "c": 1}
PLAIN = (("x", "l", "y"), ("y", "l", "x"))
SWAPPED = (("x", "l", "y"), ("y", "x", "l"))


def own_bits():
    me = lax.axis_index(AXIS)
    return me, {name: lax.rem(me // weight, 2) for name, weight in WEIGHT.items()}


def index_of(**bits):
    return sum(bits[name] * weight for name, weight in WEIGHT.items())


def flip(bit, other):
    return bit + other - 2 * bit * other


def remote(src, dst, send_sem, recv_sem, device):
    return pltpu.make_async_remote_copy(src_ref=src, dst_ref=dst, send_sem=send_sem, recv_sem=recv_sem, device_id=(device,), device_id_type=MESH)


def wait_bytes(ref, sem):
    pltpu.make_async_copy(ref, ref, sem).wait()


def loop(count, body, **kw):
    def step(i, carry):
        body(i)
        return carry
    lax.fori_loop(0, count, step, 0, **kw)


def tiles():
    return [pl.ds(i * LANES, LANES) for i in range(WIDTH // LANES)]


def clear(ref):
    ref[:] = jnp.zeros_like(ref)


def bank_of(k, issue):
    @pl.when(k < CHUNKS_A)
    def _():
        issue("attn", OWN_A, k // SUB_A, lax.rem(k, SUB_A))

    @pl.when(k >= CHUNKS_A)
    def _():
        local = k - CHUNKS_A
        issue("mlp", OWN_M, local // SUB_M, lax.rem(local, SUB_M))


def row_group(k):
    return jnp.where(k < CHUNKS_A, k // SUB_A, CHUNKS_A // SUB_A + (k - CHUNKS_A) // SUB_M)


def block_at(ref, rg, column):
    return ref.at[pl.ds(pl.multiple_of(rg * ROWS, ROWS), ROWS), pl.ds(pl.multiple_of(column, LANES), WIDTH)]


def adam(gs, w, m, v, clip):
    clipped = clip * gs
    new_m = BETA_FIRST * m + (1.0 - BETA_FIRST) * clipped
    new_v = BETA_SECOND * v + (1.0 - BETA_SECOND) * (clipped * clipped)
    u = (new_m * FIRST_SCALE) / (jnp.sqrt(new_v * SECOND_SCALE) + EPSILON) + WEIGHT_DECAY * w
    return u, new_m, new_v


def to_others(me, start_one):
    loop(GROUP - 1, lambda i: start_one(lax.rem(me + 1 + i, GROUP)))


def wide_shift(g):
    return WIDE_LANE + WIDE_ROWS * g


def wide_back(g):
    return (LANES - wide_shift(g)) % LANES


def rolled(x, shift):
    return pltpu.roll(x, shift, 1) if shift else x


def pack_state(vec_ref, wide_ref, flat, square, fill):
    clear(flat)
    flat[:, :VEC_ROWS] = vec_ref[:]
    clear(square)
    square[:WIDE_ROWS, :WIDE_COLS] = wide_ref[:]
    wide_t = square[:].T
    wide = sum(rolled(wide_t[SUBLANES * g:SUBLANES * (g + 1)], wide_shift(g)) for g in range(4))
    vec = flat[:]
    lane = lax.broadcasted_iota(jnp.int32, vec.shape, 1)
    packed = jnp.concatenate([vec[:, :LANES], vec[:, LANES:] + wide], axis=1)
    return jnp.where(jnp.logical_and(lane >= VEC_ROWS, lane < LANES + WIDE_LANE), fill, packed)


def unpack_state(packed, vec_ref, wide_ref, square):
    vec_ref[:] = packed[:, :VEC_ROWS]
    clear(square)
    for g in range(4):
        square[SUBLANES * g:SUBLANES * (g + 1), :] = rolled(packed[:, LANES:], wide_back(g))
    wide_ref[:] = square[:].T[:WIDE_ROWS, :WIDE_COLS]


def pack_grads(g_vec, g_wide, g_small, big, long):
    clear(big)
    big[:VEC_ROWS, :] = g_vec[0].astype(F32)
    clear(long)
    long[:WIDE_ROWS, :] = g_wide[0].astype(F32)
    vec = big[:].T
    wide_t = long[:].T.reshape(GROUP, 4, SUBLANES, LANES)
    wide = sum(rolled(wide_t[:, g].reshape(GROUP * SUBLANES, LANES), wide_shift(g)) for g in range(4))
    g_small[:, :, :LANES] = vec[:, :LANES].reshape(GROUP, SUBLANES, LANES).astype(BF16)
    g_small[:, :, LANES:] = (vec[:, LANES:] + wide).reshape(GROUP, SUBLANES, LANES).astype(BF16)


def unpack_replica(small_all, rep_vec, rep_wide):
    rep_vec[:] = small_all[:].astype(F32).reshape(GROUP * SUBLANES, 2 * LANES).T[:VEC_ROWS].astype(BF16)
    upper = small_all[:, :, LANES:].astype(F32).reshape(GROUP * SUBLANES, LANES)
    parts = [rolled(upper, wide_back(g)).reshape(GROUP, 1, SUBLANES, LANES) for g in range(4)]
    rep_wide[:] = jnp.concatenate(parts, axis=1).reshape(GROUP * WIDE_COLS, LANES).T[:WIDE_ROWS].astype(BF16)


def step_kernel(g_attn, g_mlp, g_vec, g_wide, w_attn, w_mlp, m_attn, m_mlp, v_attn, v_mlp, w_vec, w_wide, m_vec, m_wide, v_vec, v_wide,
                land, nw, nm, nv, rep_vec, rep_wide, nw_vec, nw_wide, nm_vec, nm_wide, nv_vec, nv_wide,
                acc1, s2buf, s3buf, s4buf, gsum, g_small, small_in, small_all, small_new, state_small, big, long, flat, square,
                msg, inboxes, rows_w, rows_u, ratio, clip_tile, n_acc,
                s1_send, s1_recv, s2_send, s2_recv, s3_send, s3_recv, s4_send, s4_recv, d_send, d_recv, load_sem, misc_send, misc_recv):
    me, bits = own_bits()
    grads = {"attn": g_attn, "mlp": g_mlp}
    states = {"attn": (w_attn, m_attn, v_attn), "mlp": (w_mlp, m_mlp, v_mlp)}

    def peer(name):
        return index_of(**{**bits, name: 1 - bits[name]})

    barrier = pltpu.get_barrier_semaphore()
    to_others(me, lambda i: pl.semaphore_signal(barrier, inc=1, device_id=(i,), device_id_type=MESH))

    def load_state(k):
        def issue(bank, own, rg, sub):
            for i, dst in enumerate((nw, nm, nv)):
                pltpu.make_async_copy(block_at(states[bank][i], rg, sub * WIDTH), dst.at[k], load_sem.at[i]).start()
        bank_of(k, issue)

    pl.semaphore_wait(barrier, GROUP - 1)

    def first_start(j, t, order):
        k = 2 * j + t
        one, two, three = order

        def issue(bank, own, rg, sub):
            def body(b):
                for da in range(2):
                    for dc in range(2):
                        target = {one: flip(bits[one], da), "c": flip(bits["c"], dc)}
                        owner = index_of(**target, **{two: b // 4, three: lax.rem(b // 2, 2), "h": lax.rem(b, 2)})
                        src = block_at(grads[bank].at[0], rg, owner * own + sub * WIDTH)
                        dst = land.at[k, (da * 2 + dc) * 8 + b]
                        if da or dc:
                            remote(src, dst, s1_send.at[k], s1_recv.at[k], index_of(**{**bits, **target})).start()
                        else:
                            pltpu.make_async_copy(src, dst, s1_recv.at[k]).start()
            loop(8, body)
        bank_of(k, issue)

    def first_finish(j, t, order):
        k = 2 * j + t
        slot = lax.rem(j, SLOTS) * 2 + t

        @pl.when(j >= SLOTS)
        def _():
            wait_bytes(s2buf.at[k - 2 * SLOTS], s2_send.at[k - 2 * SLOTS])
        wait_bytes(land.at[k], s1_recv.at[k])

        def body(b):
            for cols in tiles():
                own, core, far, both = [land[k, p * 8 + b, :, cols].astype(F32) for p in range(4)]
                acc1[slot, b, :, cols] = (own + core) + (far + both)
        loop(8, body)
        remote(acc1.at[slot, pl.ds((1 - bits[order[1]]) * 4, 4)], s2buf.at[k], s2_send.at[k], s2_recv.at[k], peer(order[1])).start()

    def second_finish(j, t, order):
        k = 2 * j + t
        slot = lax.rem(j, SLOTS) * 2 + t
        two, three = bits[order[1]], bits[order[2]]
        wait_bytes(s2buf.at[k], s2_recv.at[k])

        def body(b):
            for cols in tiles():
                s2buf[k, b, :, cols] = s2buf[k, b, :, cols] + acc1[slot, two * 4 + b, :, cols]
        loop(4, body)
        remote(s2buf.at[k, pl.ds((1 - three) * 2, 2)], s3buf.at[k], s3_send.at[k], s3_recv.at[k], peer(order[2])).start()

    def third_finish(j, t, order):
        k = 2 * j + t
        wait_bytes(s3buf.at[k], s3_recv.at[k])
        for b in range(2):
            for cols in tiles():
                s3buf[k, b, :, cols] = s3buf[k, b, :, cols] + s2buf[k, bits[order[2]] * 2 + b, :, cols]
        remote(s3buf.at[k, 1 - bits["h"]], s4buf.at[k], s4_send.at[k], s4_recv.at[k], peer("h")).start()

    def fourth_finish(j, t, order):
        k = 2 * j + t
        wait_bytes(s4buf.at[k], s4_recv.at[k])
        total = n_acc[:]
        for cols in tiles():
            gs = (s3buf[k, bits["h"], :, cols] + s4buf[k, :, cols]) * (1.0 / GROUP)
            gsum[k, :, cols] = gs
            total = total + gs * gs
        n_acc[:] = total

    def reduce_done(j, t, order):
        k = 2 * j + t
        wait_bytes(land.at[k, :24], s1_send.at[k])

        @pl.when(j >= PAIRS - SLOTS)
        def _():
            wait_bytes(s2buf.at[k], s2_send.at[k])
        wait_bytes(s3buf.at[k], s3_send.at[k])
        wait_bytes(s4buf.at[k], s4_send.at[k])

    def pair(stage, j, plain):
        for orders, chosen in ((PLAIN, plain), (SWAPPED, jnp.logical_not(plain))):
            @pl.when(chosen)
            def _():
                for t, order in enumerate(orders):
                    stage(j, t, order)

    for j in range(AHEAD):
        for t, order in enumerate(PLAIN):
            first_start(j, t, order)

    loop(CHUNKS, load_state)

    pack_grads(g_vec, g_wide, g_small, big, long)
    to_others(me, lambda i: remote(g_small.at[i], small_in.at[me], misc_send.at[0], misc_recv.at[0], i).start())
    small_in[me] = g_small[me]

    for i, (vec_ref, wide_ref, fill) in enumerate(((w_vec, w_wide, 1.0), (m_vec, m_wide, 0.0), (v_vec, v_wide, 1.0))):
        state_small[i] = pack_state(vec_ref, wide_ref, flat, square, fill)
    for i, ref in enumerate((nw, nm, nv)):
        wait_bytes(ref, load_sem.at[i])
    clear(n_acc)
    clear(rows_w)
    clear(rows_u)

    def weight_squares(k):
        total = rows_w[row_group(k)]
        for cols in tiles():
            w = nw[k, :, cols]
            total = total + w * w
        rows_w[row_group(k)] = total
    loop(CHUNKS, weight_squares)

    def reduce_step(j):
        @pl.when(j + AHEAD < PAIRS)
        def _():
            pair(first_start, j + AHEAD, j + AHEAD < PAIRS - TAIL)
        for lag, stage in zip(REDUCE_LAGS, (first_finish, second_finish, third_finish, fourth_finish, reduce_done)):
            @pl.when(jnp.logical_and(j >= lag, j < PAIRS + lag))
            def _():
                pair(stage, j - lag, j - lag < PAIRS - TAIL)
    loop(PAIRS + max(REDUCE_LAGS), reduce_step)

    wait_bytes(small_in.at[:GROUP - 1], misc_recv.at[0])
    wait_bytes(small_in.at[:GROUP - 1], misc_send.at[0])
    gs_small = jnp.sum(small_in[:].astype(F32), axis=0) * (1.0 / GROUP)

    sub_iota = lax.broadcasted_iota(jnp.int32, msg.shape[1:], 0)
    square_shape = (ROW_COUNT, LANES)
    eye = lax.broadcasted_iota(jnp.int32, square_shape, 0) == lax.broadcasted_iota(jnp.int32, square_shape, 1)

    def to_row(column_parts):
        sums = jnp.sum(column_parts, axis=1, keepdims=True)
        return jnp.sum(jnp.where(eye, jnp.broadcast_to(sums, square_shape), 0.0), axis=0, keepdims=True)

    def halves(small):
        sums = jnp.sum(small, axis=0, keepdims=True)
        return sums[:, :LANES], sums[:, LANES:]

    def sum_over_devices(rows, slot):
        inbox = inboxes.at[slot]
        value = sum(jnp.where(sub_iota == i, jnp.broadcast_to(row, sub_iota.shape), 0.0) for i, row in enumerate(rows))
        msg[slot] = value
        inbox[me] = value
        to_others(me, lambda i: remote(msg.at[slot], inbox.at[me], misc_send.at[1 + slot], misc_recv.at[1 + slot], i).start())
        wait_bytes(inbox.at[:GROUP - 1], misc_recv.at[1 + slot])
        wait_bytes(inbox.at[:GROUP - 1], misc_send.at[1 + slot])
        total = jnp.sum(inbox[:], axis=0)
        return [total[i:i + 1] for i in range(4)]

    small_w = state_small[0]
    low, high = halves(gs_small * gs_small)
    square_row = jnp.sum(n_acc[:], axis=0, keepdims=True) + low + high
    w_large, w_low, w_high, squares = sum_over_devices((to_row(rows_w[:].reshape(square_shape)), *halves(small_w * small_w), square_row), 0)
    clip = jnp.minimum(1.0, MAX_NORM / jnp.sqrt(jnp.sum(squares, axis=1, keepdims=True)))
    clip_tile[:] = jnp.broadcast_to(clip, clip_tile.shape)

    def direction(k):
        cl = clip_tile[:]
        total = rows_u[row_group(k)]
        for cols in tiles():
            u, m1, v1 = adam(gsum[k, :, cols], nw[k, :, cols], nm[k, :, cols], nv[k, :, cols], cl)
            nm[k, :, cols] = m1
            nv[k, :, cols] = v1
            gsum[k, :, cols] = u
            total = total + u * u
        rows_u[row_group(k)] = total
    loop(CHUNKS, direction)
    u_small, m1_small, v1_small = adam(gs_small, small_w, state_small[1], state_small[2], jnp.broadcast_to(clip, small_w.shape))
    u_large, u_low, u_high, _ = sum_over_devices((to_row(rows_u[:].reshape(square_shape)), *halves(u_small * u_small)), 1)

    ratio_row = jnp.sqrt(w_large) / jnp.sqrt(u_large)
    ratio_col = jnp.sum(jnp.where(eye, jnp.broadcast_to(ratio_row, square_shape), 0.0), axis=1, keepdims=True)
    ratio[:] = jnp.broadcast_to(LEARN_RATE * ratio_col, square_shape).reshape(ratio.shape)

    lane = lax.broadcasted_iota(jnp.int32, (1, LANES), 1)

    def small_ratio(w_sums, u_sums):
        return jnp.broadcast_to(LEARN_RATE * (jnp.sqrt(w_sums) / jnp.sqrt(u_sums)), (SUBLANES, LANES))

    def with_wide_totals(upper):
        wide = jnp.where(lane >= WIDE_LANE, upper, 0.0)
        for shift in (64, 32, 16):
            wide = wide + rolled(wide, shift)
        return jnp.where(lane >= WIDE_LANE, wide, upper)

    def span(k, order, depth):
        names = (order[0], "c", order[1], order[2], "h")[:depth]
        size = GROUP >> depth
        start = sum(bits[name] * (GROUP >> (i + 1)) for i, name in enumerate(names))
        return land.at[k, pl.ds(start, size)]

    def gather_high(j, t, order):
        k = 2 * j + t
        mine = span(k, order, 5)
        rr = ratio[row_group(k)]
        for cols in tiles():
            w1 = nw[k, :, cols] - rr * gsum[k, :, cols]
            nw[k, :, cols] = w1
            mine[0, :, cols] = w1.astype(BF16)
        remote(mine, mine, s4_send.at[k], s4_recv.at[k], peer("h")).start()

    def gather_three(j, t, order):
        k = 2 * j + t
        wait_bytes(land.at[k, :1], s4_recv.at[k])
        part = span(k, order, 4)
        remote(part, part, s3_send.at[k], s3_recv.at[k], peer(order[2])).start()

    def gather_two(j, t, order):
        k = 2 * j + t
        wait_bytes(land.at[k, :2], s3_recv.at[k])
        part = span(k, order, 3)
        remote(part, part, s2_send.at[k], s2_recv.at[k], peer(order[1])).start()

    def gather_one(j, t, order):
        k = 2 * j + t
        wait_bytes(land.at[k, :4], s2_recv.at[k])
        part = span(k, order, 2)
        remote(part, part, s1_send.at[k], s1_recv.at[k], peer(order[0])).start()
        remote(part, part, d_send.at[k], d_recv.at[k], peer("c")).start()

    def gather_core(j, t, order):
        k = 2 * j + t
        wait_bytes(land.at[k, :8], s1_recv.at[k])
        part = land.at[k, pl.ds((1 - bits[order[0]]) * 16 + bits["c"] * 8, 8)]
        remote(part, part, d_send.at[k], d_recv.at[k], peer("c")).start()


    def gather_done(j, t, order):
        k = 2 * j + t
        for size, sem in ((16, d_recv), (16, d_send), (8, s1_send), (4, s2_send), (2, s3_send), (1, s4_send)):
            wait_bytes(land.at[k, :size], sem.at[k])

    r_small = jnp.concatenate([small_ratio(w_low, u_low), small_ratio(with_wide_totals(w_high), with_wide_totals(u_high))], axis=1)
    state_small[0] = small_w - r_small * u_small
    state_small[1] = m1_small
    state_small[2] = v1_small
    small_new[:] = state_small[0].astype(BF16)
    small_all[me] = small_new[:]

    def gather_step(j):
        for lag, stage in zip(GATHER_LAGS, (gather_high, gather_three, gather_two, gather_one, gather_core, gather_done)):
            @pl.when(jnp.logical_and(j >= lag, j < PAIRS + lag))
            def _():
                pair(stage, j - lag, j - lag >= HEAD)

        @pl.when(j == 4)
        def _():
            to_others(me, lambda i: remote(small_new, small_all.at[me], misc_send.at[3], misc_recv.at[3], i).start())
            for i, refs in enumerate(((nw_vec, nw_wide), (nm_vec, nm_wide), (nv_vec, nv_wide))):
                unpack_state(state_small[i], *refs, square)

        @pl.when(j == PAIRS)
        def _():
            wait_bytes(small_all.at[:GROUP - 1], misc_recv.at[3])
            wait_bytes(small_all.at[:GROUP - 1], misc_send.at[3])
            unpack_replica(small_all, rep_vec, rep_wide)
    loop(PAIRS + max(GATHER_LAGS), gather_step)


def store_kernel(land, nw, nm, nv, *refs):
    small, large_out, small_out, sem = refs[:8], refs[8:16], refs[16:24], refs[24]
    outs = {"attn": large_out[::2], "mlp": large_out[1::2]}
    for i in range(8):
        pltpu.make_async_copy(small[i], small_out[i], sem.at[4 + i]).start()

    def store_pair(j, orders):
        for t, order in enumerate(orders):
            k = 2 * j + t

            def issue(bank, own, rg, sub):
                base = sub * WIDTH
                for q in range(GROUP):
                    names = (order[0], "c", order[1], order[2], "h")
                    owner = index_of(**{name: q * (2 << i) // GROUP % 2 for i, name in enumerate(names)})
                    pltpu.make_async_copy(land.at[k, q], block_at(outs[bank][0], rg, base + owner * own), sem.at[0]).start()
                for i, ref in enumerate((nw, nm, nv)):
                    pltpu.make_async_copy(ref.at[k], block_at(outs[bank][1 + i], rg, base), sem.at[1 + i]).start()
            bank_of(k, issue)
    loop(HEAD, lambda j: store_pair(j, SWAPPED))
    loop(PAIRS - HEAD, lambda j: store_pair(j + HEAD, PLAIN))
    wait_bytes(land, sem.at[0])
    for i, ref in enumerate((nw, nm, nv)):
        wait_bytes(ref, sem.at[1 + i])
    for i in range(8):
        pltpu.make_async_copy(small[i], small_out[i], sem.at[4 + i]).wait()


def solution(mesh):
    grad_spec = P(AXIS, None, None)
    shard_spec = P(None, AXIS)
    full_spec = P(None, None)
    hbm = pl.BlockSpec(memory_space=pl.ANY)
    in_vmem = pl.BlockSpec(memory_space=pltpu.VMEM)
    vmem, dma = pltpu.VMEM, pltpu.SemaphoreType.DMA
    block = (CHUNKS, ROWS, WIDTH)
    packed = (SUBLANES, 2 * LANES)
    small_shapes = [((VEC_ROWS, OWN_M // GROUP), BF16), ((WIDE_ROWS, WIDE_COLS * GROUP), BF16)] + [((SUBLANES, VEC_ROWS), F32), ((WIDE_ROWS, WIDE_COLS), F32)] * 3

    def local_step(g_attn, g_mlp, g_wide, g_vec, w_attn, w_mlp, w_wide, w_vec, m_attn, m_mlp, m_wide, m_vec, v_attn, v_mlp, v_wide, v_vec):
        scratch = [vmem((2 * SLOTS, 8, ROWS, WIDTH), F32), vmem((CHUNKS, 4, ROWS, WIDTH), F32), vmem((CHUNKS, 2, ROWS, WIDTH), F32), vmem(block, F32), vmem(block, F32)]
        scratch += [vmem((GROUP, *packed), BF16)] * 3 + [vmem(packed, BF16), vmem((3, *packed), F32)]
        scratch += [vmem((2 * LANES, GROUP * SUBLANES), F32), vmem((LANES, GROUP * WIDE_COLS), F32), vmem(packed, F32), vmem((LANES, LANES), F32)]
        scratch += [vmem((2, 4, LANES), F32), vmem((2, GROUP, 4, LANES), F32)] + [vmem((GROUPS, ROWS, LANES), F32)] * 3 + [vmem((ROWS, LANES), F32)] * 2
        scratch += [dma((CHUNKS,))] * 10 + [dma((3,)), dma((4,)), dma((4,))]
        results = pl.pallas_call(
            step_kernel,
            out_shape=[vmem((CHUNKS, GROUP, ROWS, WIDTH), BF16)] + [vmem(block, F32)] * 3 + [vmem(*item) for item in small_shapes],
            in_specs=[hbm] * 2 + [in_vmem] * 2 + [hbm] * 6 + [in_vmem] * 6,
            out_specs=[in_vmem] * 12,
            scratch_shapes=scratch,
            compiler_params=pltpu.CompilerParams(collective_id=0, has_side_effects=True, vmem_limit_bytes=30 * MIB),
            name="lamb_step",
        )(g_attn, g_mlp, g_vec, g_wide, w_attn, w_mlp, m_attn, m_mlp, v_attn, v_mlp, w_vec.T, w_wide, m_vec.T, m_wide, v_vec.T, v_wide)
        shards = [jax.ShapeDtypeStruct(w_attn.shape, F32), jax.ShapeDtypeStruct(w_mlp.shape, F32)] * 3
        (rep_attn, rep_mlp, nw_attn, nw_mlp, nm_attn, nm_mlp, nv_attn, nv_mlp,
         rep_vec, rep_wide, nw_vec, nw_wide, nm_vec, nm_wide, nv_vec, nv_wide) = pl.pallas_call(
            store_kernel,
            out_shape=[jax.ShapeDtypeStruct(g_attn.shape[1:], BF16), jax.ShapeDtypeStruct(g_mlp.shape[1:], BF16)] + shards + [jax.ShapeDtypeStruct(*item) for item in small_shapes],
            in_specs=[in_vmem] * 12,
            out_specs=[hbm] * 16,
            scratch_shapes=[dma((12,))],
            compiler_params=pltpu.CompilerParams(vmem_limit_bytes=MIB),
            name="store_results",
        )(*results)
        return (rep_attn, rep_mlp, rep_wide, rep_vec, nw_attn, nw_mlp, nw_wide, nw_vec.T, nm_attn, nm_mlp, nm_wide, nm_vec.T, nv_attn, nv_mlp, nv_wide, nv_vec.T)

    return jax.shard_map(local_step, mesh=mesh, in_specs=(grad_spec,) * 4 + (shard_spec,) * 12, out_specs=(full_spec,) * 4 + (shard_spec,) * 12, check_vma=False)
```

```python
import jax
import jax.numpy as jnp
from jax import lax
from jax.experimental import pallas as pl
from jax.experimental.pallas import tpu as pltpu
from jax.sharding import PartitionSpec as P

STEP_NUMBER = 10
LEARN_RATE = 0.04
BETA_FIRST = 0.9
BETA_SECOND = 0.999
EPSILON = 1e-6
WEIGHT_DECAY = 0.01
MAX_NORM = 1.0
FIRST_SCALE = 1.0 / (1.0 - BETA_FIRST ** STEP_NUMBER)
SECOND_SCALE = 1.0 / (1.0 - BETA_SECOND ** STEP_NUMBER)

AXIS = "data"
MESH = pl.DeviceIdType.MESH
F32 = jnp.float32
BF16 = jnp.bfloat16
LANES = 128
SUBLANES = 8
MIB = 1024 * 1024

GROUP = 32
ROWS = 16
WIDTH = 512
OWN_A = 2048
OWN_M = 8192
SUB_A = OWN_A // WIDTH
SUB_M = OWN_M // WIDTH
CHUNKS_A = 4 * SUB_A
CHUNKS = CHUNKS_A + 2 * SUB_M
PAIRS = CHUNKS // 2
GROUPS = 6
ROW_COUNT = GROUPS * ROWS
AHEAD = 1
SLOTS = 3
TAIL = 1
HEAD = 1
REDUCE_LAGS = (0, 1, 2, 3, 4)
GATHER_LAGS = (0, 1, 3, 5, 7, 8)
VEC_ROWS = 146
WIDE_ROWS = 16
WIDE_LANE = 64
WIDE_COLS = 32

WEIGHT = {"h": 16, "l": 8, "y": 4, "x": 2, "c": 1}
PLAIN = (("x", "l", "y"), ("y", "l", "x"))
SWAPPED = (("x", "l", "y"), ("y", "x", "l"))


def own_bits():
    me = lax.axis_index(AXIS)
    return me, {name: lax.rem(me // weight, 2) for name, weight in WEIGHT.items()}


def index_of(**bits):
    return sum(bits[name] * weight for name, weight in WEIGHT.items())


def flip(bit, other):
    return bit + other - 2 * bit * other


def remote(src, dst, send_sem, recv_sem, device):
    return pltpu.make_async_remote_copy(src_ref=src, dst_ref=dst, send_sem=send_sem, recv_sem=recv_sem, device_id=(device,), device_id_type=MESH)


def wait_bytes(ref, sem):
    pltpu.make_async_copy(ref, ref, sem).wait()


def loop(count, body, **kw):
    def step(i, carry):
        body(i)
        return carry
    lax.fori_loop(0, count, step, 0, **kw)


def tiles():
    return [pl.ds(i * LANES, LANES) for i in range(WIDTH // LANES)]


def clear(ref):
    ref[:] = jnp.zeros_like(ref)


def bank_of(k, issue):
    @pl.when(k < CHUNKS_A)
    def _():
        issue("attn", OWN_A, k // SUB_A, lax.rem(k, SUB_A))

    @pl.when(k >= CHUNKS_A)
    def _():
        local = k - CHUNKS_A
        issue("mlp", OWN_M, local // SUB_M, lax.rem(local, SUB_M))


def row_group(k):
    return jnp.where(k < CHUNKS_A, k // SUB_A, CHUNKS_A // SUB_A + (k - CHUNKS_A) // SUB_M)


def block_at(ref, rg, column):
    return ref.at[pl.ds(pl.multiple_of(rg * ROWS, ROWS), ROWS), pl.ds(pl.multiple_of(column, LANES), WIDTH)]


def adam(gs, w, m, v, clip):
    clipped = clip * gs
    new_m = BETA_FIRST * m + (1.0 - BETA_FIRST) * clipped
    new_v = BETA_SECOND * v + (1.0 - BETA_SECOND) * (clipped * clipped)
    u = (new_m * FIRST_SCALE) / (jnp.sqrt(new_v * SECOND_SCALE) + EPSILON) + WEIGHT_DECAY * w
    return u, new_m, new_v


def to_others(me, start_one):
    loop(GROUP - 1, lambda i: start_one(lax.rem(me + 1 + i, GROUP)), unroll=True)


def wide_shift(g):
    return WIDE_LANE + WIDE_ROWS * g


def wide_back(g):
    return (LANES - wide_shift(g)) % LANES


def rolled(x, shift):
    return pltpu.roll(x, shift, 1) if shift else x


def pack_state(vec_ref, wide_ref, flat, square, fill):
    clear(flat)
    flat[:, :VEC_ROWS] = vec_ref[:]
    clear(square)
    square[:WIDE_ROWS, :WIDE_COLS] = wide_ref[:]
    wide_t = square[:].T
    wide = sum(rolled(wide_t[SUBLANES * g:SUBLANES * (g + 1)], wide_shift(g)) for g in range(4))
    vec = flat[:]
    lane = lax.broadcasted_iota(jnp.int32, vec.shape, 1)
    packed = jnp.concatenate([vec[:, :LANES], vec[:, LANES:] + wide], axis=1)
    return jnp.where(jnp.logical_and(lane >= VEC_ROWS, lane < LANES + WIDE_LANE), fill, packed)


def unpack_state(packed, vec_ref, wide_ref, square):
    vec_ref[:] = packed[:, :VEC_ROWS]
    clear(square)
    for g in range(4):
        square[SUBLANES * g:SUBLANES * (g + 1), :] = rolled(packed[:, LANES:], wide_back(g))
    wide_ref[:] = square[:].T[:WIDE_ROWS, :WIDE_COLS]


def pack_grads(g_vec, g_wide, g_small, big, long):
    clear(big)
    big[:VEC_ROWS, :] = g_vec[0].astype(F32)
    clear(long)
    long[:WIDE_ROWS, :] = g_wide[0].astype(F32)
    vec = big[:].T
    wide_t = long[:].T.reshape(GROUP, 4, SUBLANES, LANES)
    wide = sum(rolled(wide_t[:, g].reshape(GROUP * SUBLANES, LANES), wide_shift(g)) for g in range(4))
    g_small[:, :, :LANES] = vec[:, :LANES].reshape(GROUP, SUBLANES, LANES).astype(BF16)
    g_small[:, :, LANES:] = (vec[:, LANES:] + wide).reshape(GROUP, SUBLANES, LANES).astype(BF16)


def unpack_replica(small_all, rep_vec, rep_wide):
    rep_vec[:] = small_all[:].astype(F32).reshape(GROUP * SUBLANES, 2 * LANES).T[:VEC_ROWS].astype(BF16)
    upper = small_all[:, :, LANES:].astype(F32).reshape(GROUP * SUBLANES, LANES)
    parts = [rolled(upper, wide_back(g)).reshape(GROUP, 1, SUBLANES, LANES) for g in range(4)]
    rep_wide[:] = jnp.concatenate(parts, axis=1).reshape(GROUP * WIDE_COLS, LANES).T[:WIDE_ROWS].astype(BF16)


def step_kernel(g_attn, g_mlp, g_vec, g_wide, w_attn, w_mlp, m_attn, m_mlp, v_attn, v_mlp, w_vec, w_wide, m_vec, m_wide, v_vec, v_wide,
                land, nw, nm, nv, rep_vec, rep_wide, nw_vec, nw_wide, nm_vec, nm_wide, nv_vec, nv_wide,
                acc1, s2buf, s3buf, s4buf, gsum, g_small, small_in, small_all, small_new, state_small, big, long, flat, square,
                msg, inboxes, rows_w, rows_u, ratio, clip_tile, n_acc,
                s1_send, s1_recv, s2_send, s2_recv, s3_send, s3_recv, s4_send, s4_recv, d_send, d_recv, load_sem, misc_send, misc_recv):
    me, bits = own_bits()
    grads = {"attn": g_attn, "mlp": g_mlp}
    states = {"attn": (w_attn, m_attn, v_attn), "mlp": (w_mlp, m_mlp, v_mlp)}

    def peer(name):
        return index_of(**{**bits, name: 1 - bits[name]})

    barrier = pltpu.get_barrier_semaphore()
    to_others(me, lambda i: pl.semaphore_signal(barrier, inc=1, device_id=(i,), device_id_type=MESH))

    def load_state(k):
        def issue(bank, own, rg, sub):
            for i, dst in enumerate((nw, nm, nv)):
                pltpu.make_async_copy(block_at(states[bank][i], rg, sub * WIDTH), dst.at[k], load_sem.at[i]).start()
        bank_of(k, issue)

    pl.semaphore_wait(barrier, GROUP - 1)

    def first_start(j, t, order):
        k = 2 * j + t
        one, two, three = order

        def issue(bank, own, rg, sub):
            def body(b):
                for da in range(2):
                    for dc in range(2):
                        target = {one: flip(bits[one], da), "c": flip(bits["c"], dc)}
                        owner = index_of(**target, **{two: b // 4, three: lax.rem(b // 2, 2), "h": lax.rem(b, 2)})
                        src = block_at(grads[bank].at[0], rg, owner * own + sub * WIDTH)
                        dst = land.at[k, (da * 2 + dc) * 8 + b]
                        if da or dc:
                            remote(src, dst, s1_send.at[k], s1_recv.at[k], index_of(**{**bits, **target})).start()
                        else:
                            pltpu.make_async_copy(src, dst, s1_recv.at[k]).start()
            loop(8, body)
        bank_of(k, issue)

    def first_finish(j, t, order):
        k = 2 * j + t
        slot = lax.rem(j, SLOTS) * 2 + t

        @pl.when(j >= SLOTS)
        def _():
            wait_bytes(s2buf.at[k - 2 * SLOTS], s2_send.at[k - 2 * SLOTS])
        wait_bytes(land.at[k], s1_recv.at[k])

        def body(b):
            for cols in tiles():
                own, core, far, both = [land[k, p * 8 + b, :, cols].astype(F32) for p in range(4)]
                acc1[slot, b, :, cols] = (own + core) + (far + both)
        loop(8, body)
        remote(acc1.at[slot, pl.ds((1 - bits[order[1]]) * 4, 4)], s2buf.at[k], s2_send.at[k], s2_recv.at[k], peer(order[1])).start()

    def second_finish(j, t, order):
        k = 2 * j + t
        slot = lax.rem(j, SLOTS) * 2 + t
        two, three = bits[order[1]], bits[order[2]]
        wait_bytes(s2buf.at[k], s2_recv.at[k])

        def body(b):
            for cols in tiles():
                s2buf[k, b, :, cols] = s2buf[k, b, :, cols] + acc1[slot, two * 4 + b, :, cols]
        loop(4, body)
        remote(s2buf.at[k, pl.ds((1 - three) * 2, 2)], s3buf.at[k], s3_send.at[k], s3_recv.at[k], peer(order[2])).start()

    def third_finish(j, t, order):
        k = 2 * j + t
        wait_bytes(s3buf.at[k], s3_recv.at[k])
        for b in range(2):
            for cols in tiles():
                s3buf[k, b, :, cols] = s3buf[k, b, :, cols] + s2buf[k, bits[order[2]] * 2 + b, :, cols]
        remote(s3buf.at[k, 1 - bits["h"]], s4buf.at[k], s4_send.at[k], s4_recv.at[k], peer("h")).start()

    def fourth_finish(j, t, order):
        k = 2 * j + t
        wait_bytes(s4buf.at[k], s4_recv.at[k])
        total = n_acc[:]
        for cols in tiles():
            gs = (s3buf[k, bits["h"], :, cols] + s4buf[k, :, cols]) * (1.0 / GROUP)
            gsum[k, :, cols] = gs
            total = total + gs * gs
        n_acc[:] = total

    def reduce_done(j, t, order):
        k = 2 * j + t
        wait_bytes(land.at[k, :24], s1_send.at[k])

        @pl.when(j >= PAIRS - SLOTS)
        def _():
            wait_bytes(s2buf.at[k], s2_send.at[k])
        wait_bytes(s3buf.at[k], s3_send.at[k])
        wait_bytes(s4buf.at[k], s4_send.at[k])

    def pair(stage, j, plain):
        for orders, chosen in ((PLAIN, plain), (SWAPPED, jnp.logical_not(plain))):
            @pl.when(chosen)
            def _():
                for t, order in enumerate(orders):
                    stage(j, t, order)

    for j in range(AHEAD):
        for t, order in enumerate(PLAIN):
            first_start(j, t, order)

    loop(CHUNKS, load_state)

    pack_grads(g_vec, g_wide, g_small, big, long)
    to_others(me, lambda i: remote(g_small.at[i], small_in.at[me], misc_send.at[0], misc_recv.at[0], i).start())
    small_in[me] = g_small[me]

    for i, (vec_ref, wide_ref, fill) in enumerate(((w_vec, w_wide, 1.0), (m_vec, m_wide, 0.0), (v_vec, v_wide, 1.0))):
        state_small[i] = pack_state(vec_ref, wide_ref, flat, square, fill)
    for i, ref in enumerate((nw, nm, nv)):
        wait_bytes(ref, load_sem.at[i])
    clear(n_acc)
    clear(rows_w)
    clear(rows_u)

    def weight_squares(k):
        total = rows_w[row_group(k)]
        for cols in tiles():
            w = nw[k, :, cols]
            total = total + w * w
        rows_w[row_group(k)] = total
    loop(CHUNKS, weight_squares)

    def reduce_step(j):
        @pl.when(j + AHEAD < PAIRS)
        def _():
            pair(first_start, j + AHEAD, j + AHEAD < PAIRS - TAIL)
        for lag, stage in zip(REDUCE_LAGS, (first_finish, second_finish, third_finish, fourth_finish, reduce_done)):
            @pl.when(jnp.logical_and(j >= lag, j < PAIRS + lag))
            def _():
                pair(stage, j - lag, j - lag < PAIRS - TAIL)
    loop(PAIRS + max(REDUCE_LAGS), reduce_step)

    wait_bytes(small_in.at[:GROUP - 1], misc_recv.at[0])
    wait_bytes(small_in.at[:GROUP - 1], misc_send.at[0])
    gs_small = jnp.sum(small_in[:].astype(F32), axis=0) * (1.0 / GROUP)

    sub_iota = lax.broadcasted_iota(jnp.int32, msg.shape[1:], 0)
    square_shape = (ROW_COUNT, LANES)
    eye = lax.broadcasted_iota(jnp.int32, square_shape, 0) == lax.broadcasted_iota(jnp.int32, square_shape, 1)

    def to_row(column_parts):
        sums = jnp.sum(column_parts, axis=1, keepdims=True)
        return jnp.sum(jnp.where(eye, jnp.broadcast_to(sums, square_shape), 0.0), axis=0, keepdims=True)

    def halves(small):
        sums = jnp.sum(small, axis=0, keepdims=True)
        return sums[:, :LANES], sums[:, LANES:]

    def sum_over_devices(rows, slot):
        inbox = inboxes.at[slot]
        value = sum(jnp.where(sub_iota == i, jnp.broadcast_to(row, sub_iota.shape), 0.0) for i, row in enumerate(rows))
        msg[slot] = value
        inbox[me] = value
        to_others(me, lambda i: remote(msg.at[slot], inbox.at[me], misc_send.at[1 + slot], misc_recv.at[1 + slot], i).start())
        wait_bytes(inbox.at[:GROUP - 1], misc_recv.at[1 + slot])
        total = jnp.sum(inbox[:], axis=0)
        return [total[i:i + 1] for i in range(4)]

    small_w = state_small[0]
    low, high = halves(gs_small * gs_small)
    square_row = jnp.sum(n_acc[:], axis=0, keepdims=True) + low + high
    w_large, w_low, w_high, squares = sum_over_devices((to_row(rows_w[:].reshape(square_shape)), *halves(small_w * small_w), square_row), 0)
    clip = jnp.minimum(1.0, MAX_NORM / jnp.sqrt(jnp.sum(squares, axis=1, keepdims=True)))
    clip_tile[:] = jnp.broadcast_to(clip, clip_tile.shape)

    def direction(k):
        cl = clip_tile[:]
        total = rows_u[row_group(k)]
        for cols in tiles():
            u, m1, v1 = adam(gsum[k, :, cols], nw[k, :, cols], nm[k, :, cols], nv[k, :, cols], cl)
            nm[k, :, cols] = m1
            nv[k, :, cols] = v1
            gsum[k, :, cols] = u
            total = total + u * u
        rows_u[row_group(k)] = total
    loop(CHUNKS, direction)
    u_small, m1_small, v1_small = adam(gs_small, small_w, state_small[1], state_small[2], jnp.broadcast_to(clip, small_w.shape))
    u_large, u_low, u_high, _ = sum_over_devices((to_row(rows_u[:].reshape(square_shape)), *halves(u_small * u_small)), 1)

    ratio_row = jnp.sqrt(w_large) / jnp.sqrt(u_large)
    ratio_col = jnp.sum(jnp.where(eye, jnp.broadcast_to(ratio_row, square_shape), 0.0), axis=1, keepdims=True)
    ratio[:] = jnp.broadcast_to(LEARN_RATE * ratio_col, square_shape).reshape(ratio.shape)

    lane = lax.broadcasted_iota(jnp.int32, (1, LANES), 1)

    def small_ratio(w_sums, u_sums):
        return jnp.broadcast_to(LEARN_RATE * (jnp.sqrt(w_sums) / jnp.sqrt(u_sums)), (SUBLANES, LANES))

    def with_wide_totals(upper):
        wide = jnp.where(lane >= WIDE_LANE, upper, 0.0)
        for shift in (64, 32, 16):
            wide = wide + rolled(wide, shift)
        return jnp.where(lane >= WIDE_LANE, wide, upper)

    def span(k, order, depth):
        names = (order[0], "c", order[1], order[2], "h")[:depth]
        size = GROUP >> depth
        start = sum(bits[name] * (GROUP >> (i + 1)) for i, name in enumerate(names))
        return land.at[k, pl.ds(start, size)]

    def gather_high(j, t, order):
        k = 2 * j + t
        mine = span(k, order, 5)
        rr = ratio[row_group(k)]
        for cols in tiles():
            w1 = nw[k, :, cols] - rr * gsum[k, :, cols]
            nw[k, :, cols] = w1
            mine[0, :, cols] = w1.astype(BF16)
        remote(mine, mine, s4_send.at[k], s4_recv.at[k], peer("h")).start()

    def gather_three(j, t, order):
        k = 2 * j + t
        wait_bytes(land.at[k, :1], s4_recv.at[k])
        part = span(k, order, 4)
        remote(part, part, s3_send.at[k], s3_recv.at[k], peer(order[2])).start()

    def gather_two(j, t, order):
        k = 2 * j + t
        wait_bytes(land.at[k, :2], s3_recv.at[k])
        part = span(k, order, 3)
        remote(part, part, s2_send.at[k], s2_recv.at[k], peer(order[1])).start()

    def gather_one(j, t, order):
        k = 2 * j + t
        wait_bytes(land.at[k, :4], s2_recv.at[k])
        part = span(k, order, 2)
        remote(part, part, s1_send.at[k], s1_recv.at[k], peer(order[0])).start()
        remote(part, part, d_send.at[k], d_recv.at[k], peer("c")).start()

    def gather_core(j, t, order):
        k = 2 * j + t
        wait_bytes(land.at[k, :8], s1_recv.at[k])
        part = land.at[k, pl.ds((1 - bits[order[0]]) * 16 + bits["c"] * 8, 8)]
        remote(part, part, d_send.at[k], d_recv.at[k], peer("c")).start()


    def gather_done(j, t, order):
        k = 2 * j + t
        for size, sem in ((16, d_recv), (16, d_send), (8, s1_send), (4, s2_send), (2, s3_send), (1, s4_send)):
            wait_bytes(land.at[k, :size], sem.at[k])

    r_small = jnp.concatenate([small_ratio(w_low, u_low), small_ratio(with_wide_totals(w_high), with_wide_totals(u_high))], axis=1)
    state_small[0] = small_w - r_small * u_small
    state_small[1] = m1_small
    state_small[2] = v1_small
    small_new[:] = state_small[0].astype(BF16)
    small_all[me] = small_new[:]

    def gather_step(j):
        for lag, stage in zip(GATHER_LAGS, (gather_high, gather_three, gather_two, gather_one, gather_core, gather_done)):
            @pl.when(jnp.logical_and(j >= lag, j < PAIRS + lag))
            def _():
                pair(stage, j - lag, j - lag >= HEAD)

        @pl.when(j == 4)
        def _():
            to_others(me, lambda i: remote(small_new, small_all.at[me], misc_send.at[3], misc_recv.at[3], i).start())
            for i, refs in enumerate(((nw_vec, nw_wide), (nm_vec, nm_wide), (nv_vec, nv_wide))):
                unpack_state(state_small[i], *refs, square)

        @pl.when(j == PAIRS)
        def _():
            wait_bytes(small_all.at[:GROUP - 1], misc_recv.at[3])
            wait_bytes(small_all.at[:GROUP - 1], misc_send.at[3])
            unpack_replica(small_all, rep_vec, rep_wide)
    loop(PAIRS + max(GATHER_LAGS), gather_step)
    for slot in range(2):
        wait_bytes(inboxes.at[slot, :GROUP - 1], misc_send.at[1 + slot])


def store_kernel(land, nw, nm, nv, *refs):
    small, large_out, small_out, sem = refs[:8], refs[8:16], refs[16:24], refs[24]
    outs = {"attn": large_out[::2], "mlp": large_out[1::2]}
    for i in range(8):
        pltpu.make_async_copy(small[i], small_out[i], sem.at[4 + i]).start()

    def store_pair(j, orders):
        for t, order in enumerate(orders):
            k = 2 * j + t

            def issue(bank, own, rg, sub):
                base = sub * WIDTH
                for q in range(GROUP):
                    names = (order[0], "c", order[1], order[2], "h")
                    owner = index_of(**{name: q * (2 << i) // GROUP % 2 for i, name in enumerate(names)})
                    pltpu.make_async_copy(land.at[k, q], block_at(outs[bank][0], rg, base + owner * own), sem.at[0]).start()
                for i, ref in enumerate((nw, nm, nv)):
                    pltpu.make_async_copy(ref.at[k], block_at(outs[bank][1 + i], rg, base), sem.at[1 + i]).start()
            bank_of(k, issue)
    loop(HEAD, lambda j: store_pair(j, SWAPPED))
    loop(PAIRS - HEAD, lambda j: store_pair(j + HEAD, PLAIN))
    wait_bytes(land, sem.at[0])
    for i, ref in enumerate((nw, nm, nv)):
        wait_bytes(ref, sem.at[1 + i])
    for i in range(8):
        pltpu.make_async_copy(small[i], small_out[i], sem.at[4 + i]).wait()


def solution(mesh):
    grad_spec = P(AXIS, None, None)
    shard_spec = P(None, AXIS)
    full_spec = P(None, None)
    hbm = pl.BlockSpec(memory_space=pl.ANY)
    in_vmem = pl.BlockSpec(memory_space=pltpu.VMEM)
    vmem, dma = pltpu.VMEM, pltpu.SemaphoreType.DMA
    block = (CHUNKS, ROWS, WIDTH)
    packed = (SUBLANES, 2 * LANES)
    small_shapes = [((VEC_ROWS, OWN_M // GROUP), BF16), ((WIDE_ROWS, WIDE_COLS * GROUP), BF16)] + [((SUBLANES, VEC_ROWS), F32), ((WIDE_ROWS, WIDE_COLS), F32)] * 3

    def local_step(g_attn, g_mlp, g_wide, g_vec, w_attn, w_mlp, w_wide, w_vec, m_attn, m_mlp, m_wide, m_vec, v_attn, v_mlp, v_wide, v_vec):
        scratch = [vmem((2 * SLOTS, 8, ROWS, WIDTH), F32), vmem((CHUNKS, 4, ROWS, WIDTH), F32), vmem((CHUNKS, 2, ROWS, WIDTH), F32), vmem(block, F32), vmem(block, F32)]
        scratch += [vmem((GROUP, *packed), BF16)] * 3 + [vmem(packed, BF16), vmem((3, *packed), F32)]
        scratch += [vmem((2 * LANES, GROUP * SUBLANES), F32), vmem((LANES, GROUP * WIDE_COLS), F32), vmem(packed, F32), vmem((LANES, LANES), F32)]
        scratch += [vmem((2, 4, LANES), F32), vmem((2, GROUP, 4, LANES), F32)] + [vmem((GROUPS, ROWS, LANES), F32)] * 3 + [vmem((ROWS, LANES), F32)] * 2
        scratch += [dma((CHUNKS,))] * 10 + [dma((3,)), dma((4,)), dma((4,))]
        results = pl.pallas_call(
            step_kernel,
            out_shape=[vmem((CHUNKS, GROUP, ROWS, WIDTH), BF16)] + [vmem(block, F32)] * 3 + [vmem(*item) for item in small_shapes],
            in_specs=[hbm] * 2 + [in_vmem] * 2 + [hbm] * 6 + [in_vmem] * 6,
            out_specs=[in_vmem] * 12,
            scratch_shapes=scratch,
            compiler_params=pltpu.CompilerParams(collective_id=0, has_side_effects=True, vmem_limit_bytes=30 * MIB),
            name="lamb_step",
        )(g_attn, g_mlp, g_vec, g_wide, w_attn, w_mlp, m_attn, m_mlp, v_attn, v_mlp, w_vec.T, w_wide, m_vec.T, m_wide, v_vec.T, v_wide)
        shards = [jax.ShapeDtypeStruct(w_attn.shape, F32), jax.ShapeDtypeStruct(w_mlp.shape, F32)] * 3
        (rep_attn, rep_mlp, nw_attn, nw_mlp, nm_attn, nm_mlp, nv_attn, nv_mlp,
         rep_vec, rep_wide, nw_vec, nw_wide, nm_vec, nm_wide, nv_vec, nv_wide) = pl.pallas_call(
            store_kernel,
            out_shape=[jax.ShapeDtypeStruct(g_attn.shape[1:], BF16), jax.ShapeDtypeStruct(g_mlp.shape[1:], BF16)] + shards + [jax.ShapeDtypeStruct(*item) for item in small_shapes],
            in_specs=[in_vmem] * 12,
            out_specs=[hbm] * 16,
            scratch_shapes=[dma((12,))],
            compiler_params=pltpu.CompilerParams(vmem_limit_bytes=MIB),
            name="store_results",
        )(*results)
        return (rep_attn, rep_mlp, rep_wide, rep_vec, nw_attn, nw_mlp, nw_wide, nw_vec.T, nm_attn, nm_mlp, nm_wide, nm_vec.T, nv_attn, nv_mlp, nv_wide, nv_vec.T)

    return jax.shard_map(local_step, mesh=mesh, in_specs=(grad_spec,) * 4 + (shard_spec,) * 12, out_specs=(full_spec,) * 4 + (shard_spec,) * 12, check_vma=False)
```
